32 devices in a mesh: sx: 8 (over y, x, core), sy: 4 (over z).
Axes of the slice: x: 2, y: 2, z: 4, core: 2. Of those that a mesh axis runs over, the one named last changes fastest.
Arguments:
- vectors: bfloat16 [64, 64, 128, 128], P(None, 'sx', 'sy'), may hold values from -0.4453125 to 0.4453125
- root_stiff: float32 [64, 128, 128], P('sx', 'sy'), may hold values from 0.5 to 2
- diag_coef: float32 [64, 128, 128], P('sx', 'sy'), may hold values from -3 to 3
- counts: int32 [8, 4], P('sx', 'sy'), may hold values from 8 to 64, as said below
Outputs:
- own_block: float32 [8, 4, 64, 64], P('sx', 'sy')
- face_blocks: float32 [8, 4, 64, 256], P('sx', 'sy')
- corner_blocks: float32 [8, 4, 64, 256], P('sx', 'sy')
- offsets: int32 [8, 4], P('sx', 'sy')
The draws below stay inside these ranges and needn't reach their ends.
Inputs may be any that keep to these rules, and one draw needn't show every extreme that they name: Some subdomain has exactly 64 eigenvectors in every draw; small counts are more common than large ones.
All inputs are finite; a program needn't handle non-finite values.
Results may differ from the reference program's by a relative error of at most 0.007.
Values may be sent and summed in bfloat16 or wider, within the bound.
No kernel may reach another device: no remote copies, remote signals or barrier semaphores. Data moves between devices by JAX's collectives and lax.ppermute only.
A program may use at most 128 MiB of HBM per device.

```python
import math
import jax
import jax.numpy as jnp
from jax import lax

KMAX = 64
KMIN = 8
CX = 8
CY = 32
CZ = 128
SUB_X = 8
SUB_Y = 4
NX = 64
NY = 128
N_SX = 8
N_SY = 4


def draw_counts(key, part):
    key_one, key_two, key_three = jax.random.split(jax.random.fold_in(key, 11), 3)
    spread = KMAX - KMIN
    draw_one = jax.random.randint(key_one, (N_SX, N_SY), 0, spread + 1)
    draw_two = jax.random.randint(key_two, (N_SX, N_SY), 0, spread + 1)
    skewed = KMIN + draw_one * draw_two // max(spread, 1)
    chosen = jax.random.randint(key_three, (), 0, N_SX * N_SY)
    linear = skewed.reshape(-1)
    linear = jnp.where(jnp.arange(N_SX * N_SY) == chosen, KMAX, linear)
    return linear.reshape(N_SX, N_SY).astype(jnp.int32)


def shard_levels(own_key, shape, cuts, low, largest):
    gain, own = 1.0, jax.random.fold_in(own_key, 6)
    for position, parts in cuts:
        steps = jnp.exp(jax.random.uniform(jax.random.fold_in(own, position), (parts,), jnp.float32, low / len(cuts), largest / len(cuts)))
        gain = gain * jnp.repeat(steps, shape[position] // parts).reshape([-1 if axis == position else 1 for axis in range(len(shape))])
    return gain


def bell_draw(own_key, extent, width, bound, pieces=(), kind=jnp.bfloat16):
    loudness = shard_levels(own_key, extent, pieces, -0.22, 0.18) if pieces else 1.0
    values = jax.random.normal(own_key, extent, jnp.float32) * width * loudness
    return jnp.minimum(jnp.maximum(values, -bound), bound).astype(kind)


def setup_inputs(seed: int = 0) -> dict:
    seeds = jax.random.split(jax.random.key(seed), 5)
    vectors = bell_draw(seeds[0], (KMAX, NX, NY, CZ), (1.0 / (CX * CY * CZ) ** 0.25), 0.4453125, ((1, 8), (2, 4)))
    root_stiff = jnp.clip(jnp.exp(math.log(2.0) - 1.3862944 * jax.random.uniform(seeds[1], (NX, NY, CZ), jnp.float32) ** shard_levels(seeds[1], (NX, NY, CZ), ((0, 8), (1, 4)), -0.2, 0.2)), 0.5, 2.0)
    diag_coef = jnp.clip(jax.random.uniform(seeds[2], (NX, NY, CZ), jnp.float32, -3.0, 3.0) * shard_levels(seeds[2], (NX, NY, CZ), ((0, 8), (1, 4)), -0.4, 0.0), -3.0, 3.0)
    counts = draw_counts(jax.random.fold_in(seeds[4], 71), 0)
    return {"vectors": vectors, "root_stiff": root_stiff, "diag_coef": diag_coef, "counts": counts}


def smooth_along(values, dim_index):
    length = values.shape[dim_index]
    zero_slab = jnp.zeros_like(lax.slice_in_dim(values, 0, 1, axis=dim_index))
    below_side = jnp.concatenate([zero_slab, lax.slice_in_dim(values, 0, length - 1, axis=dim_index)], axis=dim_index)
    above_side = jnp.concatenate([lax.slice_in_dim(values, 1, length, axis=dim_index), zero_slab], axis=dim_index)
    return values + 0.5 * (below_side + above_side)


def own_term(masked, scaled, stiff_here, diag_here):
    scaled_wide = scaled.astype(jnp.float32)
    smoothed = smooth_along(smooth_along(smooth_along(scaled_wide, 1), 2), 3)
    beside = smoothed - scaled_wide
    applied = (diag_here[None] * masked.astype(jnp.float32) - stiff_here[None] * beside).astype(jnp.bfloat16)
    vec_rows = masked.shape[0]
    return lax.dot_general(masked.reshape(vec_rows, -1), applied.reshape(vec_rows, -1), (((1,), (1,)), ((), ())), preferred_element_type=jnp.float32)


def face_term(own_layer, near_layer):
    weighted = 0.5 * smooth_along(smooth_along(near_layer.astype(jnp.float32), 1), 2)
    vec_rows = own_layer.shape[0]
    return -lax.dot_general(own_layer.astype(jnp.float32).reshape(vec_rows, -1), weighted.reshape(vec_rows, -1), (((1,), (1,)), ((), ())), precision=lax.Precision.HIGHEST, preferred_element_type=jnp.float32)


def corner_term(own_column, near_column):
    weighted = 0.25 * smooth_along(near_column.astype(jnp.float32), 1)
    return -lax.dot_general(own_column.astype(jnp.float32), weighted, (((1,), (1,)), ((), ())), precision=lax.Precision.HIGHEST, preferred_element_type=jnp.float32)


def reference(vectors, root_stiff, diag_coef, counts):
    vec_rows = vectors.shape[0]

    def scaled_piece(sub_x, sub_y, x_start, x_len, y_start, y_len):
        inside = (sub_x >= 0) & (sub_x < SUB_X) & (sub_y >= 0) & (sub_y < SUB_Y)
        clamp_x = jnp.clip(sub_x, 0, SUB_X - 1).astype(jnp.int32)
        clamp_y = jnp.clip(sub_y, 0, SUB_Y - 1).astype(jnp.int32)
        start_x = (clamp_x * CX + x_start).astype(jnp.int32)
        start_y = (clamp_y * CY + y_start).astype(jnp.int32)
        zero_start = jnp.zeros((), jnp.int32)
        piece = lax.dynamic_slice(vectors, (zero_start, start_x, start_y, zero_start), (vec_rows, x_len, y_len, CZ))
        stiff = lax.dynamic_slice(root_stiff, (start_x, start_y, zero_start), (x_len, y_len, CZ))
        live_count = counts[clamp_x, clamp_y]
        row_index = lax.broadcasted_iota(jnp.int32, (vec_rows, 1, 1, 1), 0)
        keep = (row_index < live_count) & inside
        masked = jnp.where(keep, piece, jnp.zeros_like(piece))
        scaled = (stiff[None] * masked.astype(jnp.float32)).astype(jnp.bfloat16)
        return masked, scaled, stiff

    def one_subdomain(flat_index):
        sub_x = flat_index // SUB_Y
        sub_y = flat_index % SUB_Y
        masked, scaled, stiff_here = scaled_piece(sub_x, sub_y, 0, CX, 0, CY)
        zero_start = jnp.zeros((), jnp.int32)
        diag_here = lax.dynamic_slice(diag_coef, ((sub_x * CX).astype(jnp.int32), (sub_y * CY).astype(jnp.int32), zero_start), (CX, CY, CZ))
        own_block = own_term(masked, scaled, stiff_here, diag_here)
        faces = []
        for step_x in (-1, 1):
            own_layer = scaled[:, CX - 1 if step_x > 0 else 0]
            near_layer = scaled_piece(sub_x + step_x, sub_y, 0 if step_x > 0 else CX - 1, 1, 0, CY)[1][:, 0]
            faces.append(face_term(own_layer, near_layer))
        for step_y in (-1, 1):
            own_layer = scaled[:, :, CY - 1 if step_y > 0 else 0]
            near_layer = scaled_piece(sub_x, sub_y + step_y, 0, CX, 0 if step_y > 0 else CY - 1, 1)[1][:, :, 0]
            faces.append(face_term(own_layer, near_layer))
        corners = []
        for step_x in (-1, 1):
            for step_y in (-1, 1):
                own_column = scaled[:, CX - 1 if step_x > 0 else 0, CY - 1 if step_y > 0 else 0]
                near_column = scaled_piece(sub_x + step_x, sub_y + step_y, 0 if step_x > 0 else CX - 1, 1, 0 if step_y > 0 else CY - 1, 1)[1][:, 0, 0]
                corners.append(corner_term(own_column, near_column))
        return own_block, jnp.concatenate(faces, axis=1), jnp.concatenate(corners, axis=1)

    own_all, face_all, corner_all = lax.map(one_subdomain, jnp.arange(SUB_X * SUB_Y, dtype=jnp.int32))
    offsets = (jnp.cumsum(counts, axis=1) - counts).astype(jnp.int32)
    return (own_all.reshape(SUB_X, SUB_Y, vec_rows, vec_rows), face_all.reshape(SUB_X, SUB_Y, vec_rows, 4 * vec_rows), corner_all.reshape(SUB_X, SUB_Y, vec_rows, 4 * vec_rows), offsets)
```

```python
import jax
import jax.numpy as jnp
from jax import lax
from jax.experimental import pallas as pl
from jax.experimental.pallas import tpu as pltpu
from jax.sharding import PartitionSpec as P

F32 = jnp.float32
BF = jnp.bfloat16
NT = (((1,), (1,)), ((), ()))
NN = (((1,), (0,)), ((), ()))
PAD = 4
VM = pl.BlockSpec(memory_space=pltpu.VMEM)
SM = pl.BlockSpec(memory_space=pltpu.SMEM)
ANY = pl.BlockSpec(memory_space=pl.ANY)


def cost(flops, bytes_accessed):
    return pl.CostEstimate(flops=flops, bytes_accessed=bytes_accessed, transcendentals=0)


def tri(n, reps, scale):
    size = n * reps
    i = lax.broadcasted_iota(jnp.int32, (size, size), 0)
    j = lax.broadcasted_iota(jnp.int32, (size, size), 1)
    near = ((i // n) == (j // n)) & (jnp.abs(i - j) == 1)
    return (jnp.where(i == j, 1.0, jnp.where(near, 0.5, 0.0)) * scale).astype(BF)


def even(axis):
    return lax.rem(lax.axis_index(axis), 2) == 0


def pairs(count, first):
    steps = []
    for i in range(first, count - 1, 2):
        steps += [(i, i + 1), (i + 1, i)]
    return steps


def edge_kernel(cnt, v, s, fxa, fxb, fxc, fya, fyb, xbuf, ybuf, rx, ry, xsem, ysem):
    _, rows, ny, nz = xbuf.shape
    nx, band = ybuf.shape[2], ybuf.shape[3]
    stx, sty = ny + PAD, band + PAD
    x_even, y_even = even("sx"), even("sy")
    xa = jnp.where(x_even, nx - 1, 0)
    xb = nx - 1 - xa
    ya = jnp.where(y_even, ny - band, 0)
    yb = ny - band - ya
    xcopies = [pltpu.make_async_copy(v.at[:, x], xbuf.at[i], xsem.at[i]) for i, x in enumerate((xb, xa))]
    ycopies = [
        pltpu.make_async_copy(v.at[:, :, pl.ds(pl.multiple_of(y, band), band)], ybuf.at[i], ysem.at[i])
        for i, y in enumerate((ya, yb))
    ]
    for c in xcopies + ycopies:
        c.start()
    live = lax.broadcasted_iota(jnp.int32, (rows, nz), 0) < cnt[0, 0]

    def scaled(m, stiff):
        return jnp.where(live, m * jnp.broadcast_to(stiff, (rows, nz)), 0.0).astype(BF)

    for i, (x, out) in enumerate(((xb, fxb), (xa, fxa))):
        xcopies[i].wait()
        for a in range(rows):
            rx[a * stx : a * stx + ny, :] = xbuf[i, a].astype(F32)
        for y in range(ny):
            out[y] = scaled(rx[pl.ds(y, rows, stride=stx), :], s[x, pl.ds(y, 1), :])
        if i == 0:
            fxc[0] = fxb[jnp.where(y_even, ny - 1, 0)]
            fxc[1] = fxb[jnp.where(y_even, 0, ny - 1)]
    for i, (y0, out) in enumerate(((ya, fya), (yb, fyb))):
        ycopies[i].wait()
        inner = jnp.where(y0 == 0, 0, band - 1)
        for x in range(nx):
            for a in range(rows):
                ry[x, a * sty : a * sty + band, :] = ybuf[i, a, x].astype(F32)
            out[x] = scaled(ry[x, pl.ds(inner, rows, stride=sty), :], s[x, pl.ds(y0 + inner, 1), :])


def edges(counts, vectors, stiff):
    rows, nx, ny, nz = vectors.shape
    band = 16
    face = lambda *dims: jax.ShapeDtypeStruct((*dims, rows, nz), BF)
    return pl.pallas_call(
        edge_kernel,
        out_shape=(face(ny), face(ny), face(2), face(nx), face(nx)),
        in_specs=[SM, ANY, VM],
        out_specs=(VM,) * 5,
        scratch_shapes=[
            pltpu.VMEM((2, rows, ny, nz), BF),
            pltpu.VMEM((2, rows, nx, band, nz), BF),
            pltpu.VMEM((rows * (ny + PAD), nz), F32),
            pltpu.VMEM((nx, rows * (band + PAD), nz), F32),
            pltpu.SemaphoreType.DMA((2,)),
            pltpu.SemaphoreType.DMA((2,)),
        ],
        cost_estimate=cost(10**6, 4 * 10**6),
        name="edges",
    )(counts, vectors, stiff)


def pack_kernel(known, fya, fyb, rxa, rxc, mya, myb, sem):
    nx, rows, nz = fya.shape
    ny = rxa.shape[0]
    y_even = even("sy")
    hi = jnp.where(y_even, ny - 1, 0)
    copies = [
        pltpu.make_async_copy(rxa.at[y], out.at[nx], sem.at[i])
        for i, (y, out) in enumerate(((hi, mya), (ny - 1 - hi, myb)))
    ]
    for c in copies:
        c.start()
    lane = lax.broadcasted_iota(jnp.int32, (rows, nz), 1)
    counts = jnp.zeros((rows, nz), F32)
    for i in range(known.shape[1]):
        counts = jnp.where(lane == i, known[0, i].astype(F32), counts)
    for i, (src, out) in enumerate(((fya, mya), (fyb, myb))):
        out[0:nx] = src[...]
        out[nx + 1] = rxc[i]
        out[nx + 2] = counts.astype(BF)
    for c in copies:
        c.wait()


def pack(known, fya, fyb, rxa, rxc):
    nx, rows, nz = fya.shape
    out = jax.ShapeDtypeStruct((nx + 3, rows, nz), BF)
    return pl.pallas_call(
        pack_kernel,
        out_shape=(out, out),
        in_specs=[SM, VM, VM, ANY, VM],
        out_specs=(VM, VM),
        scratch_shapes=[pltpu.SemaphoreType.DMA((2,))],
        cost_estimate=cost(10**5, 10**6),
        name="pack",
    )(known, fya, fyb, rxa, rxc)


def own_kernel(cnt, v, s, d, fxa, fxb, fya, fyb, own, wxa, wxb, wya, wyb, wc, vbuf, r, er, ubuf, pbuf, szr, acc, sem):
    nx, rows, ny, nz = vbuf.shape
    st = ny + PAD

    def copy(x):
        return pltpu.make_async_copy(v.at[:, x], vbuf.at[x], sem.at[x])

    for x in range(nx):
        copy(x).start()
    er[...] = d[...] + s[...] * s[...]
    ubuf[...] = jnp.zeros_like(ubuf)
    acc[...] = jnp.zeros_like(acc)
    szr[...] = tri(nz, 2, -0.25)

    def along_z(stack, n):
        wide = jnp.concatenate([jnp.concatenate([stack(2 * c), stack(2 * c + 1)], 1) for c in range(n // 2)], 0)
        z = lax.dot_general(wide, szr[...], NN, preferred_element_type=F32)
        return [z[(i // 2) * rows : (i // 2 + 1) * rows, (i % 2) * nz : (i % 2 + 1) * nz] for i in range(n)]

    def smooth_part(total):
        zs = along_z(lambda y: pbuf[y], ny)
        for c in range(ny // 2):
            left = jnp.concatenate([zs[2 * c].astype(BF), zs[2 * c + 1].astype(BF)], 1)
            right = jnp.concatenate([pbuf[2 * c], pbuf[2 * c + 1]], 1)
            total += lax.dot_general(left, right, NT, preferred_element_type=F32)
        last = lax.dot_general(pbuf[ny], szr[0:nz, 0:nz], NN, preferred_element_type=F32).astype(BF)
        return total + lax.dot_general(last, pbuf[ny], NT, preferred_element_type=F32)

    @pl.loop(0, nx)
    def _(x):
        copy(x).wait()
        for a in range(rows):
            r[a * st : a * st + ny, :] = vbuf[x, a].astype(F32)
        total = acc[...]
        last = None
        left, right = [], []
        for y in range(ny):
            m = r[pl.ds(y, rows, stride=st), :]
            stiff = jnp.broadcast_to(s[x, pl.ds(y, 1), :], (rows, nz))
            centre = jnp.broadcast_to(er[x, pl.ds(y, 1), :], (rows, nz))
            u = (m * stiff).astype(BF)
            left.append((m * centre).astype(BF))
            right.append(m.astype(BF))
            both = u + ubuf[y]
            ubuf[y] = u
            pbuf[y] = both if last is None else both + last
            last = both
            if y % 2:
                total += lax.dot_general(
                    jnp.concatenate(left, 1), jnp.concatenate(right, 1), NT, preferred_element_type=F32
                )
                left, right = [], []
        pbuf[ny] = last
        acc[...] = smooth_part(total)

    last = None
    for y in range(ny):
        both = ubuf[y]
        pbuf[y] = both if last is None else both + last
        last = both
    pbuf[ny] = last
    total = smooth_part(acc[...])
    live = cnt[0, 0]
    keep = (lax.broadcasted_iota(jnp.int32, (rows, rows), 0) < live) & (
        lax.broadcasted_iota(jnp.int32, (rows, rows), 1) < live
    )
    own[...] = jnp.where(keep, total, 0.0)

    for src, out in ((fxa, wxa), (fxb, wxb), (fya, wya), (fyb, wyb)):
        n = src.shape[0]
        zs = along_z(lambda i: src[i], n)
        for i in range(n):
            t = zs[i] + zs[i]
            if i > 0:
                t = t + zs[i - 1]
            if i < n - 1:
                t = t + zs[i + 1]
            out[i] = t.astype(BF)
    y_even = even("sy")
    rows_y = (jnp.where(y_even, ny - 1, 0), jnp.where(y_even, 0, ny - 1))
    for i, src in enumerate((fxa, fxb)):
        zs = along_z(lambda k: src[rows_y[k]], 2)
        for k in range(2):
            wc[2 * i + k] = zs[k].astype(BF)


def own(counts, vectors, stiff, diag, fxa, fxb, fya, fyb):
    rows, nx, ny, nz = vectors.shape
    face = lambda n: jax.ShapeDtypeStruct((n, rows, nz), BF)
    return pl.pallas_call(
        own_kernel,
        out_shape=(jax.ShapeDtypeStruct((rows, rows), F32), face(ny), face(ny), face(nx), face(nx), face(4)),
        in_specs=[SM, ANY, VM, VM, VM, VM, VM, VM],
        out_specs=(VM,) * 6,
        scratch_shapes=[
            pltpu.VMEM((nx, rows, ny, nz), BF),
            pltpu.VMEM((rows * (ny + PAD), nz), F32),
            pltpu.VMEM((nx, ny, nz), F32),
            pltpu.VMEM((ny, rows, nz), BF),
            pltpu.VMEM((ny + 1, rows, nz), BF),
            pltpu.VMEM((2 * nz, 2 * nz), BF),
            pltpu.VMEM((rows, rows), F32),
            pltpu.SemaphoreType.DMA((nx,)),
        ],
        cost_estimate=cost(2 * 10**9, 8 * 10**6),
        name="own",
    )(counts, vectors, stiff, diag, fxa, fxb, fya, fyb)


def couple_kernel(masks, cnt, wxa, wxb, wya, wyb, wc, rxa, rxb, rya, ryb, known, faces, corners, offsets):
    nx, rows, nz = wya.shape
    x_even, y_even = even("sx"), even("sy")

    def gram(left, right, n):
        total = jnp.zeros((rows, rows), F32)
        for i in range(0, n, 2):
            total += lax.dot_general(
                jnp.concatenate([left[i], left[i + 1]], 1),
                jnp.concatenate([right[i], right[i + 1]], 1),
                NT,
                preferred_element_type=F32,
            )
        return total

    ya, yb = gram(wya, rya, nx), gram(wyb, ryb, nx)
    around = [
        [lax.dot_general(wc[2 * i + k], ry[nx + i], NT, preferred_element_type=F32) for k, ry in enumerate((rya, ryb))]
        for i in range(2)
    ]
    n = wxa.shape[0]
    xa, xb = gram(wxa, rxa, n), gram(wxb, rxb, n)
    parts = (
        jnp.where(x_even, xb, xa),
        jnp.where(x_even, xa, xb),
        jnp.where(y_even, yb, ya),
        jnp.where(y_even, ya, yb),
    )
    for i, part in enumerate(parts):
        faces[:, i * rows : (i + 1) * rows] = part
    for ix in range(2):
        for iy in range(2):
            options = [
                jnp.where(y_even == (iy == 1), around[k][0], around[k][1]) for k in range(2)
            ]
            i = 2 * ix + iy
            corners[:, i * rows : (i + 1) * rows] = jnp.where(x_even == (ix == 1), options[0], options[1])

    me = lax.axis_index("sy")
    total = jnp.int32(0)
    for i, mask in enumerate(masks):
        total += jnp.where((me ^ mask) < me, known[0, i], 0)
    lane = lax.broadcasted_iota(jnp.int32, (8, nz), 1)
    theirs = rya[nx + 2, 0:16].astype(F32)[0:8]
    picked = jnp.zeros((8, nz), F32)
    for i, mask in enumerate(masks):
        picked = jnp.where((lane == i) & ((me ^ (mask ^ 1)) < me), theirs, picked)
    offsets[...] = jnp.sum(picked[0:1], axis=1, keepdims=True).astype(jnp.int32) + total


def couple(masks, counts, ws, received, known):
    wxa = ws[0]
    rows, nz = wxa.shape[1:]
    block = jax.ShapeDtypeStruct((rows, 4 * rows), F32)
    return pl.pallas_call(
        lambda *refs: couple_kernel(masks, *refs),
        out_shape=(block, block, jax.ShapeDtypeStruct((1, 1), jnp.int32)),
        in_specs=[SM] + [VM] * 9 + [SM],
        out_specs=(VM, VM, VM),
        cost_estimate=cost(10**8, 3 * 10**6),
        name="couple",
    )(counts, *ws, *received, known)


def on_device(vectors, root_stiff, diag_coef, counts):
    n_x, n_y = lax.axis_size("sx"), lax.axis_size("sy")
    fxa, fxb, fxc, fya, fyb = edges(counts, vectors, root_stiff)
    rxc = lax.ppermute(fxc, "sx", pairs(n_x, 1))
    rxb = lax.ppermute(fxb, "sx", pairs(n_x, 1))
    rxa = lax.ppermute(fxa, "sx", pairs(n_x, 0))
    known, masks, bit = counts, [0], n_y // 2
    while bit >= 2:
        other = lax.ppermute(known, "sy", [(i, i ^ bit) for i in range(n_y)])
        known = jnp.concatenate([known, other], axis=1)
        masks += [m ^ bit for m in masks]
        bit //= 2
    mya, myb = pack(known, fya, fyb, rxa, rxc)
    rya = lax.ppermute(mya, "sy", pairs(n_y, 0))
    ryb = lax.ppermute(myb, "sy", pairs(n_y, 1))
    own_block, *ws = own(counts, vectors, root_stiff, diag_coef, fxa, fxb, fya, fyb)
    faces, corners, offsets = couple(tuple(masks), counts, ws, (rxa, rxb, rya, ryb), known)
    return own_block[None, None], faces[None, None], corners[None, None], offsets


def solution(mesh):
    assert mesh.shape["sy"] & (mesh.shape["sy"] - 1) == 0
    return jax.shard_map(
        on_device,
        mesh=mesh,
        in_specs=(
            P(None, "sx", "sy", None),
            P("sx", "sy", None),
            P("sx", "sy", None),
            P("sx", "sy"),
        ),
        out_specs=(
            P("sx", "sy", None, None),
            P("sx", "sy", None, None),
            P("sx", "sy", None, None),
            P("sx", "sy"),
        ),
        check_vma=False,
    )
```

```python
import jax
import jax.numpy as jnp
from jax import lax
from jax.experimental import pallas as pl
from jax.experimental.pallas import tpu as pltpu
from jax.sharding import PartitionSpec as P

F32 = jnp.float32
BF = jnp.bfloat16
NT = (((1,), (1,)), ((), ()))
NN = (((1,), (0,)), ((), ()))
PAD = 4
VM = pl.BlockSpec(memory_space=pltpu.VMEM)
SM = pl.BlockSpec(memory_space=pltpu.SMEM)
ANY = pl.BlockSpec(memory_space=pl.ANY)
HBM = pl.BlockSpec(memory_space=pltpu.HBM)


def cost(flops, bytes_accessed):
    return pl.CostEstimate(flops=flops, bytes_accessed=bytes_accessed, transcendentals=0)


def tri(n, reps, scale):
    size = n * reps
    i = lax.broadcasted_iota(jnp.int32, (size, size), 0)
    j = lax.broadcasted_iota(jnp.int32, (size, size), 1)
    near = ((i // n) == (j // n)) & (jnp.abs(i - j) == 1)
    return (jnp.where(i == j, 1.0, jnp.where(near, 0.5, 0.0)) * scale).astype(BF)


def even(axis):
    return lax.rem(lax.axis_index(axis), 2) == 0


def pairs(count, first):
    steps = []
    for i in range(first, count - 1, 2):
        steps += [(i, i + 1), (i + 1, i)]
    return steps


def edge_kernel(cnt_any, v, s_any, fxa, fxb, fxc, fya, fyb, cnt, s, xbuf, ybuf, rx, ry, xsem, ysem, sem):
    small = [
        pltpu.make_async_copy(src, dst, sem.at[i]) for i, (src, dst) in enumerate(((cnt_any, cnt), (s_any, s)))
    ]
    for c in small:
        c.start()
    _, rows, ny, nz = xbuf.shape
    nx, band = ybuf.shape[2], ybuf.shape[3]
    stx, sty = ny + PAD, band + PAD
    x_even, y_even = even("sx"), even("sy")
    xa = jnp.where(x_even, nx - 1, 0)
    xb = nx - 1 - xa
    ya = jnp.where(y_even, ny - band, 0)
    yb = ny - band - ya
    xcopies = [pltpu.make_async_copy(v.at[:, x], xbuf.at[i], xsem.at[i]) for i, x in enumerate((xb, xa))]
    ycopies = [
        pltpu.make_async_copy(v.at[:, :, pl.ds(pl.multiple_of(y, band), band)], ybuf.at[i], ysem.at[i])
        for i, y in enumerate((ya, yb))
    ]
    for c in xcopies + ycopies:
        c.start()
    for c in small:
        c.wait()
    live = lax.broadcasted_iota(jnp.int32, (rows, nz), 0) < cnt[0, 0]

    def scaled(m, stiff):
        return jnp.where(live, m * jnp.broadcast_to(stiff, (rows, nz)), 0.0).astype(BF)

    for i, (x, out) in enumerate(((xb, fxb), (xa, fxa))):
        xcopies[i].wait()
        for a in range(rows):
            rx[a * stx : a * stx + ny, :] = xbuf[i, a].astype(F32)
        for y in range(ny):
            out[y] = scaled(rx[pl.ds(y, rows, stride=stx), :], s[x, pl.ds(y, 1), :])
        if i == 0:
            fxc[0] = fxb[jnp.where(y_even, ny - 1, 0)]
            fxc[1] = fxb[jnp.where(y_even, 0, ny - 1)]
    for i, (y0, out) in enumerate(((ya, fya), (yb, fyb))):
        ycopies[i].wait()
        inner = jnp.where(y0 == 0, 0, band - 1)
        for x in range(nx):
            for a in range(rows):
                ry[x, a * sty : a * sty + band, :] = ybuf[i, a, x].astype(F32)
            out[x] = scaled(ry[x, pl.ds(inner, rows, stride=sty), :], s[x, pl.ds(y0 + inner, 1), :])


def edges(counts, vectors, stiff):
    rows, nx, ny, nz = vectors.shape
    band = 16
    face = lambda *dims: jax.ShapeDtypeStruct((*dims, rows, nz), BF)
    return pl.pallas_call(
        edge_kernel,
        out_shape=(face(ny), face(ny), face(2), face(nx), face(nx)),
        in_specs=[HBM, HBM, HBM],
        out_specs=(VM,) * 5,
        scratch_shapes=[
            pltpu.SMEM((1, 1), jnp.int32),
            pltpu.VMEM(stiff.shape, F32),
            pltpu.VMEM((2, rows, ny, nz), BF),
            pltpu.VMEM((2, rows, nx, band, nz), BF),
            pltpu.VMEM((rows * (ny + PAD), nz), F32),
            pltpu.VMEM((nx, rows * (band + PAD), nz), F32),
            pltpu.SemaphoreType.DMA((2,)),
            pltpu.SemaphoreType.DMA((2,)),
            pltpu.SemaphoreType.DMA((2,)),
        ],
        cost_estimate=cost(10**6, 4 * 10**6),
        compiler_params=pltpu.CompilerParams(vmem_limit_bytes=57 * 2**20),
        name="edges",
    )(counts, vectors, stiff)


def pack_kernel(fya, fyb, rxa, rxc, *rest):
    *known, mya, myb = rest
    nx, rows, nz = fya.shape
    ny = rxa.shape[0]
    y_even = even("sy")
    hi = jnp.where(y_even, ny - 1, 0)
    lane = lax.broadcasted_iota(jnp.int32, (rows, nz), 1)
    counts = jnp.zeros((rows, nz), F32)
    for i, one in enumerate(known):
        counts = jnp.where(lane == i, one[0, 0].astype(F32), counts)
    for i, (src, y, out) in enumerate(((fya, hi, mya), (fyb, ny - 1 - hi, myb))):
        out[0:nx] = src[...]
        out[nx] = rxa[y]
        out[nx + 1] = rxc[i]
        out[nx + 2] = counts.astype(BF)


def pack(known, fya, fyb, rxa, rxc):
    nx, rows, nz = fya.shape
    out = jax.ShapeDtypeStruct((nx + 3, rows, nz), BF)
    return pl.pallas_call(
        pack_kernel,
        out_shape=(out, out),
        in_specs=[VM] * 4 + [SM] * len(known),
        out_specs=(VM, VM),
        cost_estimate=cost(10**5, 10**6),
        compiler_params=pltpu.CompilerParams(vmem_limit_bytes=8 * 2**20),
        name="pack",
    )(fya, fyb, rxa, rxc, *known)


def own_kernel(
    cnt_any, v, s, d, fxa, fxb, fya, fyb, own, wxa, wxb, wya, wyb, wc,
    cnt, r, er, ubuf, pbuf, szr, acc, small_sem,
):
    rows, nx, ny, nz = v.shape
    st = ny + PAD
    small = pltpu.make_async_copy(cnt_any, cnt, small_sem)
    small.start()
    er[...] = d[...] + s[...] * s[...]
    ubuf[...] = jnp.zeros_like(ubuf)
    acc[...] = jnp.zeros_like(acc)
    szr[...] = tri(nz, 2, -0.25)

    def along_z(stack, n):
        wide = jnp.concatenate([jnp.concatenate([stack(2 * c), stack(2 * c + 1)], 1) for c in range(n // 2)], 0)
        z = lax.dot_general(wide, szr[...], NN, preferred_element_type=F32)
        return [z[(i // 2) * rows : (i // 2 + 1) * rows, (i % 2) * nz : (i % 2 + 1) * nz] for i in range(n)]

    def smooth_part(total):
        zs = along_z(lambda y: pbuf[y], ny)
        for c in range(ny // 2):
            left = jnp.concatenate([zs[2 * c].astype(BF), zs[2 * c + 1].astype(BF)], 1)
            right = jnp.concatenate([pbuf[2 * c], pbuf[2 * c + 1]], 1)
            total += lax.dot_general(left, right, NT, preferred_element_type=F32)
        last = lax.dot_general(pbuf[ny], szr[0:nz, 0:nz], NN, preferred_element_type=F32).astype(BF)
        return total + lax.dot_general(last, pbuf[ny], NT, preferred_element_type=F32)

    @pl.loop(0, nx)
    def _(x):
        for a in range(rows):
            r[a * st : a * st + ny, :] = v[a, x].astype(F32)
        total = acc[...]
        last = None
        left, right = [], []
        for y in range(ny):
            m = r[pl.ds(y, rows, stride=st), :]
            stiff = jnp.broadcast_to(s[x, pl.ds(y, 1), :], (rows, nz))
            centre = jnp.broadcast_to(er[x, pl.ds(y, 1), :], (rows, nz))
            u = (m * stiff).astype(BF)
            left.append((m * centre).astype(BF))
            right.append(m.astype(BF))
            both = u + ubuf[y]
            ubuf[y] = u
            pbuf[y] = both if last is None else both + last
            last = both
            if y % 2:
                total += lax.dot_general(
                    jnp.concatenate(left, 1), jnp.concatenate(right, 1), NT, preferred_element_type=F32
                )
                left, right = [], []
        pbuf[ny] = last
        acc[...] = smooth_part(total)

    last = None
    for y in range(ny):
        both = ubuf[y]
        pbuf[y] = both if last is None else both + last
        last = both
    pbuf[ny] = last
    total = smooth_part(acc[...])
    small.wait()
    live = cnt[0, 0]
    keep = (lax.broadcasted_iota(jnp.int32, (rows, rows), 0) < live) & (
        lax.broadcasted_iota(jnp.int32, (rows, rows), 1) < live
    )
    own[...] = jnp.where(keep, total, 0.0)

    for src, out in ((fxa, wxa), (fxb, wxb), (fya, wya), (fyb, wyb)):
        n = src.shape[0]
        zs = along_z(lambda i: src[i], n)
        for i in range(n):
            t = zs[i] + zs[i]
            if i > 0:
                t = t + zs[i - 1]
            if i < n - 1:
                t = t + zs[i + 1]
            out[i] = t.astype(BF)
    y_even = even("sy")
    rows_y = (jnp.where(y_even, ny - 1, 0), jnp.where(y_even, 0, ny - 1))
    for i, src in enumerate((fxa, fxb)):
        zs = along_z(lambda k: src[rows_y[k]], 2)
        for k in range(2):
            wc[2 * i + k] = zs[k].astype(BF)


def own(counts, vectors, stiff, diag, fxa, fxb, fya, fyb):
    rows, nx, ny, nz = vectors.shape
    face = lambda n: jax.ShapeDtypeStruct((n, rows, nz), BF)
    return pl.pallas_call(
        own_kernel,
        out_shape=(jax.ShapeDtypeStruct((rows, rows), F32), face(ny), face(ny), face(nx), face(nx), face(4)),
        in_specs=[HBM] + [VM] * 7,
        out_specs=(VM,) * 6,
        scratch_shapes=[
            pltpu.SMEM((1, 1), jnp.int32),
            pltpu.VMEM((rows * (ny + PAD), nz), F32),
            pltpu.VMEM((nx, ny, nz), F32),
            pltpu.VMEM((ny, rows, nz), BF),
            pltpu.VMEM((ny + 1, rows, nz), BF),
            pltpu.VMEM((2 * nz, 2 * nz), BF),
            pltpu.VMEM((rows, rows), F32),
            pltpu.SemaphoreType.DMA(()),
        ],
        compiler_params=pltpu.CompilerParams(vmem_limit_bytes=16 * 2**20),
        cost_estimate=cost(2 * 10**9, 8 * 10**6),
        name="own",
    )(counts, vectors, stiff, diag, fxa, fxb, fya, fyb)


def gram(left, right, n, total):
    for i in range(0, n, 2):
        total += lax.dot_general(
            jnp.concatenate([left[i], left[i + 1]], 1),
            jnp.concatenate([right[i], right[i + 1]], 1),
            NT,
            preferred_element_type=F32,
        )
    return total


def across_x_kernel(wxa, wxb, rxa, rxb, out):
    n, rows, _ = wxa.shape
    zero = jnp.zeros((rows, rows), F32)
    xa, xb = gram(wxa, rxa, n, zero), gram(wxb, rxb, n, zero)
    x_even = even("sx")
    out[:, 0:rows] = jnp.where(x_even, xb, xa)
    out[:, rows : 2 * rows] = jnp.where(x_even, xa, xb)


def across_x(wxa, wxb, rxa, rxb):
    _, rows, _ = wxa.shape
    return pl.pallas_call(
        across_x_kernel,
        out_shape=jax.ShapeDtypeStruct((rows, 2 * rows), F32),
        in_specs=[VM] * 4,
        out_specs=VM,
        cost_estimate=cost(10**8, 2 * 10**6),
        compiler_params=pltpu.CompilerParams(vmem_limit_bytes=8 * 2**20),
        name="across_x",
    )(wxa, wxb, rxa, rxb)


def across_y_kernel(masks, fx, wya, wyb, wc, rya, ryb, *rest):
    *known, faces, corners, offsets = rest
    nx, rows, nz = wya.shape
    x_even, y_even = even("sx"), even("sy")
    zero = jnp.zeros((rows, rows), F32)
    around = [
        [lax.dot_general(wc[2 * i + k], ry[nx + i], NT, preferred_element_type=F32) for k, ry in enumerate((rya, ryb))]
        for i in range(2)
    ]
    ya, yb = gram(wya, rya, nx, zero), gram(wyb, ryb, nx, zero)
    faces[:, 0 : 2 * rows] = fx[...]
    faces[:, 2 * rows : 3 * rows] = jnp.where(y_even, yb, ya)
    faces[:, 3 * rows : 4 * rows] = jnp.where(y_even, ya, yb)
    for ix in range(2):
        for iy in range(2):
            options = [jnp.where(y_even == (iy == 1), around[k][0], around[k][1]) for k in range(2)]
            i = 2 * ix + iy
            corners[:, i * rows : (i + 1) * rows] = jnp.where(x_even == (ix == 1), options[0], options[1])

    me = lax.axis_index("sy")
    total = jnp.int32(0)
    for one, mask in zip(known, masks):
        total += jnp.where((me ^ mask) < me, one[0, 0], 0)
    lane = lax.broadcasted_iota(jnp.int32, (8, nz), 1)
    theirs = rya[nx + 2, 0:16].astype(F32)[0:8]
    picked = jnp.zeros((8, nz), F32)
    for i, mask in enumerate(masks):
        picked = jnp.where((lane == i) & ((me ^ (mask ^ 1)) < me), theirs, picked)
    offsets[...] = jnp.sum(picked[0:1], axis=1, keepdims=True).astype(jnp.int32) + total


def across_y(masks, fx, wya, wyb, wc, rya, ryb, known):
    rows = wya.shape[1]
    block = jax.ShapeDtypeStruct((rows, 4 * rows), F32)
    return pl.pallas_call(
        lambda *refs: across_y_kernel(masks, *refs),
        out_shape=(block, block, jax.ShapeDtypeStruct((1, 1), jnp.int32)),
        in_specs=[VM] * 6 + [SM] * len(known),
        out_specs=(VM, VM, VM),
        cost_estimate=cost(10**8, 10**6),
        compiler_params=pltpu.CompilerParams(vmem_limit_bytes=8 * 2**20),
        name="across_y",
    )(fx, wya, wyb, wc, rya, ryb, *known)


def swap(values, axis, first):
    return lax.ppermute(values, axis, pairs(lax.axis_size(axis), first))


def on_device(vectors, root_stiff, diag_coef, counts):
    n_y = lax.axis_size("sy")
    known, masks, bit = [counts], [0], n_y // 2
    while bit >= 2:
        known += [lax.ppermute(one, "sy", [(i, i ^ bit) for i in range(n_y)]) for one in known]
        masks += [m ^ bit for m in masks]
        bit //= 2
    fxa, fxb, fxc, fya, fyb = edges(counts, vectors, root_stiff)
    rxc = swap(fxc, "sx", 1)
    rxb = swap(fxb, "sx", 1)
    rxa = swap(fxa, "sx", 0)
    own_block, wxa, wxb, wya, wyb, wc = own(counts, vectors, root_stiff, diag_coef, fxa, fxb, fya, fyb)
    mya, myb = pack(known, fya, fyb, rxa, rxc)
    rya = swap(mya, "sy", 0)
    ryb = swap(myb, "sy", 1)
    fx = across_x(wxa, wxb, rxa, rxb)
    faces, corners, offsets = across_y(tuple(masks), fx, wya, wyb, wc, rya, ryb, known)
    return own_block[None, None], faces[None, None], corners[None, None], offsets


def solution(mesh):
    assert mesh.shape["sy"] & (mesh.shape["sy"] - 1) == 0
    return jax.shard_map(
        on_device,
        mesh=mesh,
        in_specs=(
            P(None, "sx", "sy", None),
            P("sx", "sy", None),
            P("sx", "sy", None),
            P("sx", "sy"),
        ),
        out_specs=(
            P("sx", "sy", None, None),
            P("sx", "sy", None, None),
            P("sx", "sy", None, None),
            P("sx", "sy"),
        ),
        check_vma=False,
    )
```

```python
import jax
import jax.numpy as jnp
from jax import lax
from jax.experimental import pallas as pl
from jax.experimental.pallas import tpu as pltpu
from jax.sharding import PartitionSpec as P

F32 = jnp.float32
BF = jnp.bfloat16
NT = (((1,), (1,)), ((), ()))
NN = (((1,), (0,)), ((), ()))
PAD = 4
BAND = 8
VM = pl.BlockSpec(memory_space=pltpu.VMEM)
SM = pl.BlockSpec(memory_space=pltpu.SMEM)
ANY = pl.BlockSpec(memory_space=pl.ANY)
HBM = pl.BlockSpec(memory_space=pltpu.HBM)


def cost(flops, bytes_accessed):
    return pl.CostEstimate(flops=flops, bytes_accessed=bytes_accessed, transcendentals=0)


def tri(n, reps, scale):
    size = n * reps
    i = lax.broadcasted_iota(jnp.int32, (size, size), 0)
    j = lax.broadcasted_iota(jnp.int32, (size, size), 1)
    near = ((i // n) == (j // n)) & (jnp.abs(i - j) == 1)
    return (jnp.where(i == j, 1.0, jnp.where(near, 0.5, 0.0)) * scale).astype(BF)


def even(axis):
    return lax.rem(lax.axis_index(axis), 2) == 0


def pairs(count, first):
    steps = []
    for i in range(first, count - 1, 2):
        steps += [(i, i + 1), (i + 1, i)]
    return steps


def edge_kernel(cnt_any, v, s, fxa, fxb, fxc, fya, fyb, cnt, rx, ry, sem):
    small = pltpu.make_async_copy(cnt_any, cnt, sem)
    small.start()
    rows, nx, ny, nz = v.shape
    stx, sty = ny + PAD, BAND + PAD
    x_even, y_even = even("sx"), even("sy")
    xa = jnp.where(x_even, nx - 1, 0)
    ya = jnp.where(y_even, ny - 1, 0)
    xb, yb = nx - 1 - xa, ny - 1 - ya
    small.wait()
    live = lax.broadcasted_iota(jnp.int32, (rows, nz), 0) < cnt[0, 0]

    def scaled(m, stiff):
        return jnp.where(live, m * jnp.broadcast_to(stiff, (rows, nz)), 0.0).astype(BF)

    for x, out in ((xb, fxb), (xa, fxa)):
        for a in range(rows):
            rx[a * stx : a * stx + ny, :] = v[a, x].astype(F32)
        for y in range(ny):
            out[y] = scaled(rx[pl.ds(y, rows, stride=stx), :], s[x, pl.ds(y, 1), :])
    fxc[0] = fxb[ya]
    fxc[1] = fxb[yb]
    for y, out in ((ya, fya), (yb, fyb)):
        band = pl.multiple_of((y // BAND) * BAND, BAND)
        inner = y - band
        for x in range(nx):
            for a in range(rows):
                ry[x, a * sty : a * sty + BAND, :] = v[a, x, pl.ds(band, BAND), :].astype(F32)
            out[x] = scaled(ry[x, pl.ds(inner, rows, stride=sty), :], s[x, pl.ds(y, 1), :])


def edges(counts, vectors, stiff):
    rows, nx, ny, nz = vectors.shape
    face = lambda n: jax.ShapeDtypeStruct((n, rows, nz), BF)
    return pl.pallas_call(
        edge_kernel,
        out_shape=(face(ny), face(ny), face(2), face(nx), face(nx)),
        in_specs=[HBM, VM, VM],
        out_specs=(VM,) * 5,
        scratch_shapes=[
            pltpu.SMEM((1, 1), jnp.int32),
            pltpu.VMEM((rows * (ny + PAD), nz), F32),
            pltpu.VMEM((nx, rows * (BAND + PAD), nz), F32),
            pltpu.SemaphoreType.DMA(()),
        ],
        cost_estimate=cost(10**6, 4 * 10**6),
        compiler_params=pltpu.CompilerParams(vmem_limit_bytes=12 * 2**20),
        name="edges",
    )(counts, vectors, stiff)


def pack_kernel(fya, fyb, rxa, rxc, *rest):
    *known, mya, myb = rest
    nx, rows, nz = fya.shape
    ny = rxa.shape[0]
    y_even = even("sy")
    hi = jnp.where(y_even, ny - 1, 0)
    lane = lax.broadcasted_iota(jnp.int32, (rows, nz), 1)
    counts = jnp.zeros((rows, nz), F32)
    for i, one in enumerate(known):
        counts = jnp.where(lane == i, one[0, 0].astype(F32), counts)
    for i, (src, y, out) in enumerate(((fya, hi, mya), (fyb, ny - 1 - hi, myb))):
        out[0:nx] = src[...]
        out[nx] = rxa[y]
        out[nx + 1] = rxc[i]
        out[nx + 2] = counts.astype(BF)


def pack(known, fya, fyb, rxa, rxc):
    nx, rows, nz = fya.shape
    out = jax.ShapeDtypeStruct((nx + 3, rows, nz), BF)
    return pl.pallas_call(
        pack_kernel,
        out_shape=(out, out),
        in_specs=[VM] * 4 + [SM] * len(known),
        out_specs=(VM, VM),
        cost_estimate=cost(10**5, 10**6),
        compiler_params=pltpu.CompilerParams(vmem_limit_bytes=8 * 2**20),
        name="pack",
    )(fya, fyb, rxa, rxc, *known)


def along_z(stack, n, stencil):
    rows, nz = stack(0).shape
    wide = jnp.concatenate([jnp.concatenate([stack(2 * c), stack(2 * c + 1)], 1) for c in range(n // 2)], 0)
    z = lax.dot_general(wide, stencil, NN, preferred_element_type=F32)
    return [z[(i // 2) * rows : (i // 2 + 1) * rows, (i % 2) * nz : (i % 2 + 1) * nz] for i in range(n)]


def smooth_kernel(fxa, fxb, fya, fyb, wxa, wxb, wya, wyb, wc):
    ny, _, nz = fxa.shape
    stencil = tri(nz, 2, -0.25)
    for src, out in ((fxa, wxa), (fxb, wxb), (fya, wya), (fyb, wyb)):
        n = src.shape[0]
        zs = along_z(lambda i: src[i], n, stencil)
        for i in range(n):
            t = zs[i] + zs[i]
            if i > 0:
                t = t + zs[i - 1]
            if i < n - 1:
                t = t + zs[i + 1]
            out[i] = t.astype(BF)
    y_even = even("sy")
    rows_y = (jnp.where(y_even, ny - 1, 0), jnp.where(y_even, 0, ny - 1))
    for i, src in enumerate((fxa, fxb)):
        zs = along_z(lambda k: src[rows_y[k]], 2, stencil)
        for k in range(2):
            wc[2 * i + k] = zs[k].astype(BF)


def smooth(fxa, fxb, fya, fyb):
    ny, rows, nz = fxa.shape
    nx = fya.shape[0]
    face = lambda n: jax.ShapeDtypeStruct((n, rows, nz), BF)
    return pl.pallas_call(
        smooth_kernel,
        out_shape=(face(ny), face(ny), face(nx), face(nx), face(4)),
        in_specs=[VM] * 4,
        out_specs=(VM,) * 5,
        cost_estimate=cost(10**8, 2 * 10**6),
        compiler_params=pltpu.CompilerParams(vmem_limit_bytes=12 * 2**20),
        name="smooth",
    )(fxa, fxb, fya, fyb)


def own_kernel(
    cnt_any, v, s, d, own,
    cnt, r, er, ubuf, pbuf, szr, acc, small_sem,
):
    rows, nx, ny, nz = v.shape
    st = ny + PAD
    small = pltpu.make_async_copy(cnt_any, cnt, small_sem)
    small.start()
    er[...] = d[...] + s[...] * s[...]
    ubuf[...] = jnp.zeros_like(ubuf)
    acc[...] = jnp.zeros_like(acc)
    szr[...] = tri(nz, 2, -0.25)

    def smooth_part(total):
        zs = along_z(lambda y: pbuf[y], ny, szr[...])
        for c in range(ny // 2):
            left = jnp.concatenate([zs[2 * c].astype(BF), zs[2 * c + 1].astype(BF)], 1)
            right = jnp.concatenate([pbuf[2 * c], pbuf[2 * c + 1]], 1)
            total += lax.dot_general(left, right, NT, preferred_element_type=F32)
        last = lax.dot_general(pbuf[ny], szr[0:nz, 0:nz], NN, preferred_element_type=F32).astype(BF)
        return total + lax.dot_general(last, pbuf[ny], NT, preferred_element_type=F32)

    @pl.loop(0, nx)
    def _(x):
        for a in range(rows):
            r[a * st : a * st + ny, :] = v[a, x].astype(F32)
        total = acc[...]
        last = None
        left, right = [], []
        for y in range(ny):
            m = r[pl.ds(y, rows, stride=st), :]
            stiff = jnp.broadcast_to(s[x, pl.ds(y, 1), :], (rows, nz))
            centre = jnp.broadcast_to(er[x, pl.ds(y, 1), :], (rows, nz))
            u = (m * stiff).astype(BF)
            left.append((m * centre).astype(BF))
            right.append(m.astype(BF))
            both = u + ubuf[y]
            ubuf[y] = u
            pbuf[y] = both if last is None else both + last
            last = both
            if y % 2:
                total += lax.dot_general(
                    jnp.concatenate(left, 1), jnp.concatenate(right, 1), NT, preferred_element_type=F32
                )
                left, right = [], []
        pbuf[ny] = last
        acc[...] = smooth_part(total)

    last = None
    for y in range(ny):
        both = ubuf[y]
        pbuf[y] = both if last is None else both + last
        last = both
    pbuf[ny] = last
    total = smooth_part(acc[...])
    small.wait()
    live = cnt[0, 0]
    keep = (lax.broadcasted_iota(jnp.int32, (rows, rows), 0) < live) & (
        lax.broadcasted_iota(jnp.int32, (rows, rows), 1) < live
    )
    own[...] = jnp.where(keep, total, 0.0)


def own(counts, vectors, stiff, diag):
    rows, nx, ny, nz = vectors.shape
    return pl.pallas_call(
        own_kernel,
        out_shape=jax.ShapeDtypeStruct((rows, rows), F32),
        in_specs=[HBM] + [VM] * 3,
        out_specs=VM,
        scratch_shapes=[
            pltpu.SMEM((1, 1), jnp.int32),
            pltpu.VMEM((rows * (ny + PAD), nz), F32),
            pltpu.VMEM((nx, ny, nz), F32),
            pltpu.VMEM((ny, rows, nz), BF),
            pltpu.VMEM((ny + 1, rows, nz), BF),
            pltpu.VMEM((2 * nz, 2 * nz), BF),
            pltpu.VMEM((rows, rows), F32),
            pltpu.SemaphoreType.DMA(()),
        ],
        compiler_params=pltpu.CompilerParams(vmem_limit_bytes=16 * 2**20),
        cost_estimate=cost(2 * 10**9, 8 * 10**6),
        name="own",
    )(counts, vectors, stiff, diag)


def gram(left, right, n, total):
    for i in range(0, n, 2):
        total += lax.dot_general(
            jnp.concatenate([left[i], left[i + 1]], 1),
            jnp.concatenate([right[i], right[i + 1]], 1),
            NT,
            preferred_element_type=F32,
        )
    return total


def couple_kernel(masks, wxa, wxb, wya, wyb, wc, rxa, rxb, rya, ryb, *rest):
    *known, faces, corners, offsets = rest
    nx, rows, nz = wya.shape
    x_even, y_even = even("sx"), even("sy")
    zero = jnp.zeros((rows, rows), F32)
    around = [
        [lax.dot_general(wc[2 * i + k], ry[nx + i], NT, preferred_element_type=F32) for k, ry in enumerate((rya, ryb))]
        for i in range(2)
    ]
    ya, yb = gram(wya, rya, nx, zero), gram(wyb, ryb, nx, zero)
    xa, xb = gram(wxa, rxa, wxa.shape[0], zero), gram(wxb, rxb, wxa.shape[0], zero)
    faces[:, 0:rows] = jnp.where(x_even, xb, xa)
    faces[:, rows : 2 * rows] = jnp.where(x_even, xa, xb)
    faces[:, 2 * rows : 3 * rows] = jnp.where(y_even, yb, ya)
    faces[:, 3 * rows : 4 * rows] = jnp.where(y_even, ya, yb)
    for ix in range(2):
        for iy in range(2):
            options = [jnp.where(y_even == (iy == 1), around[k][0], around[k][1]) for k in range(2)]
            i = 2 * ix + iy
            corners[:, i * rows : (i + 1) * rows] = jnp.where(x_even == (ix == 1), options[0], options[1])

    me = lax.axis_index("sy")
    total = jnp.int32(0)
    for one, mask in zip(known, masks):
        total += jnp.where((me ^ mask) < me, one[0, 0], 0)
    lane = lax.broadcasted_iota(jnp.int32, (8, nz), 1)
    theirs = rya[nx + 2, 0:16].astype(F32)[0:8]
    picked = jnp.zeros((8, nz), F32)
    for i, mask in enumerate(masks):
        picked = jnp.where((lane == i) & ((me ^ (mask ^ 1)) < me), theirs, picked)
    offsets[...] = jnp.sum(picked[0:1], axis=1, keepdims=True).astype(jnp.int32) + total


def couple(masks, ws, received, known):
    rows = ws[0].shape[1]
    block = jax.ShapeDtypeStruct((rows, 4 * rows), F32)
    return pl.pallas_call(
        lambda *refs: couple_kernel(masks, *refs),
        out_shape=(block, block, jax.ShapeDtypeStruct((1, 1), jnp.int32)),
        in_specs=[VM] * 9 + [SM] * len(known),
        out_specs=(VM, VM, VM),
        cost_estimate=cost(10**8, 10**6),
        compiler_params=pltpu.CompilerParams(vmem_limit_bytes=8 * 2**20),
        name="couple",
    )(*ws, *received, *known)


def swap(values, axis, first):
    return lax.ppermute(values, axis, pairs(lax.axis_size(axis), first))


def on_device(vectors, root_stiff, diag_coef, counts):
    n_y = lax.axis_size("sy")
    known, masks, bit = [counts], [0], n_y // 2
    while bit >= 2:
        known += [lax.ppermute(one, "sy", [(i, i ^ bit) for i in range(n_y)]) for one in known]
        masks += [m ^ bit for m in masks]
        bit //= 2
    fxa, fxb, fxc, fya, fyb = edges(counts, vectors, root_stiff)
    rxc = swap(fxc, "sx", 1)
    rxb = swap(fxb, "sx", 1)
    rxa = swap(fxa, "sx", 0)
    ws = smooth(fxa, fxb, fya, fyb)
    mya, myb = pack(known, fya, fyb, rxa, rxc)
    rya = swap(mya, "sy", 0)
    ryb = swap(myb, "sy", 1)
    own_block = own(counts, vectors, root_stiff, diag_coef)
    faces, corners, offsets = couple(tuple(masks), ws, (rxa, rxb, rya, ryb), known)
    return own_block[None, None], faces[None, None], corners[None, None], offsets


def solution(mesh):
    assert mesh.shape["sy"] & (mesh.shape["sy"] - 1) == 0
    return jax.shard_map(
        on_device,
        mesh=mesh,
        in_specs=(
            P(None, "sx", "sy", None),
            P("sx", "sy", None),
            P("sx", "sy", None),
            P("sx", "sy"),
        ),
        out_specs=(
            P("sx", "sy", None, None),
            P("sx", "sy", None, None),
            P("sx", "sy", None, None),
            P("sx", "sy"),
        ),
        check_vma=False,
    )
```

```python
import jax
import jax.numpy as jnp
from jax import lax
from jax.experimental import pallas as pl
from jax.experimental.pallas import tpu as pltpu
from jax.sharding import PartitionSpec as P

F32 = jnp.float32
BF = jnp.bfloat16
NT = (((1,), (1,)), ((), ()))
NN = (((1,), (0,)), ((), ()))
PAD = 4
BAND = 8
VM = pl.BlockSpec(memory_space=pltpu.VMEM)
SM = pl.BlockSpec(memory_space=pltpu.SMEM)
ANY = pl.BlockSpec(memory_space=pl.ANY)
HBM = pl.BlockSpec(memory_space=pltpu.HBM)


def cost(flops, bytes_accessed):
    return pl.CostEstimate(flops=flops, bytes_accessed=bytes_accessed, transcendentals=0)


def tri(n, reps, scale):
    size = n * reps
    i = lax.broadcasted_iota(jnp.int32, (size, size), 0)
    j = lax.broadcasted_iota(jnp.int32, (size, size), 1)
    near = ((i // n) == (j // n)) & (jnp.abs(i - j) == 1)
    return (jnp.where(i == j, 1.0, jnp.where(near, 0.5, 0.0)) * scale).astype(BF)


def even(axis):
    return lax.rem(lax.axis_index(axis), 2) == 0


def pairs(count, first):
    steps = []
    for i in range(first, count - 1, 2):
        steps += [(i, i + 1), (i + 1, i)]
    return steps


def edge_kernel(cnt, v, s, fxa, fxb, fxc, fya, fyb, rx, ry):
    rows, nx, ny, nz = v.shape
    stx, sty = ny + PAD, BAND + PAD
    x_even, y_even = even("sx"), even("sy")
    xa = jnp.where(x_even, nx - 1, 0)
    ya = jnp.where(y_even, ny - 1, 0)
    xb, yb = nx - 1 - xa, ny - 1 - ya
    live = lax.broadcasted_iota(jnp.int32, (rows, nz), 0) < jnp.broadcast_to(cnt[...], (rows, nz))

    def scaled(m, stiff):
        return jnp.where(live, m * jnp.broadcast_to(stiff, (rows, nz)), 0.0).astype(BF)

    for x, out in ((xb, fxb), (xa, fxa)):
        for a in range(rows):
            rx[a * stx : a * stx + ny, :] = v[a, x].astype(F32)
        for y in range(ny):
            out[y] = scaled(rx[pl.ds(y, rows, stride=stx), :], s[x, pl.ds(y, 1), :])
    fxc[0] = fxb[ya]
    fxc[1] = fxb[yb]
    for y, out in ((ya, fya), (yb, fyb)):
        band = pl.multiple_of((y // BAND) * BAND, BAND)
        inner = y - band
        for x in range(nx):
            for a in range(rows):
                ry[x, a * sty : a * sty + BAND, :] = v[a, x, pl.ds(band, BAND), :].astype(F32)
            out[x] = scaled(ry[x, pl.ds(inner, rows, stride=sty), :], s[x, pl.ds(y, 1), :])


def edges(counts, vectors, stiff):
    rows, nx, ny, nz = vectors.shape
    face = lambda n: jax.ShapeDtypeStruct((n, rows, nz), BF)
    return pl.pallas_call(
        edge_kernel,
        out_shape=(face(ny), face(ny), face(2), face(nx), face(nx)),
        in_specs=[VM, VM, VM],
        out_specs=(VM,) * 5,
        scratch_shapes=[
            pltpu.VMEM((rows * (ny + PAD), nz), F32),
            pltpu.VMEM((nx, rows * (BAND + PAD), nz), F32),
        ],
        cost_estimate=cost(10**6, 4 * 10**6),
        compiler_params=pltpu.CompilerParams(vmem_limit_bytes=12 * 2**20),
        name="edges",
    )(counts, vectors, stiff)


def pack_kernel(cnt, fya, fyb, rxa, rxc, mya, myb):
    nx, rows, nz = fya.shape
    ny = rxa.shape[0]
    hi = jnp.where(even("sy"), ny - 1, 0)
    count = jnp.broadcast_to(cnt[...].astype(F32), (rows, nz)).astype(BF)
    for i, (src, y, out) in enumerate(((fya, hi, mya), (fyb, ny - 1 - hi, myb))):
        out[0:nx] = src[...]
        out[nx] = rxa[y]
        out[nx + 1] = rxc[i]
        out[nx + 2] = count


def pack(counts, fya, fyb, rxa, rxc):
    nx, rows, nz = fya.shape
    out = jax.ShapeDtypeStruct((nx + 3, rows, nz), BF)
    return pl.pallas_call(
        pack_kernel,
        out_shape=(out, out),
        in_specs=[VM] * 5,
        out_specs=(VM, VM),
        cost_estimate=cost(10**5, 10**6),
        compiler_params=pltpu.CompilerParams(vmem_limit_bytes=8 * 2**20),
        name="pack",
    )(counts, fya, fyb, rxa, rxc)


def along_z(stack, n, stencil):
    rows, nz = stack(0).shape
    wide = jnp.concatenate([jnp.concatenate([stack(2 * c), stack(2 * c + 1)], 1) for c in range(n // 2)], 0)
    z = lax.dot_general(wide, stencil, NN, preferred_element_type=F32)
    return [z[(i // 2) * rows : (i // 2 + 1) * rows, (i % 2) * nz : (i % 2 + 1) * nz] for i in range(n)]


def smooth_kernel(fxa, fxb, fya, fyb, wxa, wxb, wya, wyb, wc):
    ny, _, nz = fxa.shape
    stencil = tri(nz, 2, -0.25)
    for src, out in ((fxa, wxa), (fxb, wxb), (fya, wya), (fyb, wyb)):
        n = src.shape[0]
        zs = along_z(lambda i: src[i], n, stencil)
        for i in range(n):
            t = zs[i] + zs[i]
            if i > 0:
                t = t + zs[i - 1]
            if i < n - 1:
                t = t + zs[i + 1]
            out[i] = t.astype(BF)
    y_even = even("sy")
    rows_y = (jnp.where(y_even, ny - 1, 0), jnp.where(y_even, 0, ny - 1))
    for i, src in enumerate((fxa, fxb)):
        zs = along_z(lambda k: src[rows_y[k]], 2, stencil)
        for k in range(2):
            wc[2 * i + k] = zs[k].astype(BF)


def smooth(fxa, fxb, fya, fyb):
    ny, rows, nz = fxa.shape
    nx = fya.shape[0]
    face = lambda n: jax.ShapeDtypeStruct((n, rows, nz), BF)
    return pl.pallas_call(
        smooth_kernel,
        out_shape=(face(ny), face(ny), face(nx), face(nx), face(4)),
        in_specs=[VM] * 4,
        out_specs=(VM,) * 5,
        cost_estimate=cost(10**8, 2 * 10**6),
        compiler_params=pltpu.CompilerParams(vmem_limit_bytes=12 * 2**20),
        name="smooth",
    )(fxa, fxb, fya, fyb)


def own_kernel(cnt, v, s, d, own, r, er, ubuf, acc, accs):
    rows, nx, ny, nz = v.shape
    st = ny + PAD
    er[...] = d[...] + s[...] * s[...]
    for ref in (ubuf, acc, accs):
        ref[...] = jnp.zeros_like(ref)
    inner = jnp.where(lax.broadcasted_iota(jnp.int32, (rows, nz), 1) == 0, 0.0, 1.0).astype(BF)

    def with_previous(p):
        return p + pltpu.roll(p, 1, 1) * inner

    def dot(left, right, total):
        return total + lax.dot_general(
            jnp.concatenate(left, 1), jnp.concatenate(right, 1), NT, preferred_element_type=F32
        )

    def slab(x, total, stotal):
        if x is not None:
            for a in range(rows):
                r[a * st : a * st + ny, :] = v[a, x].astype(F32)
        last = None
        left, right, ps = [], [], []
        for y in range(ny):
            if x is not None:
                m = r[pl.ds(y, rows, stride=st), :]
                u = (m * jnp.broadcast_to(s[x, pl.ds(y, 1), :], (rows, nz))).astype(BF)
                left.append((m * jnp.broadcast_to(er[x, pl.ds(y, 1), :], (rows, nz))).astype(BF))
                right.append(m.astype(BF))
                both = u + ubuf[y]
                ubuf[y] = u
            else:
                both = ubuf[y]
            ps.append(both if last is None else both + last)
            last = both
            if y % 2:
                if x is not None:
                    total = dot(left, right, total)
                stotal = dot([with_previous(p) for p in ps], ps, stotal)
                left, right, ps = [], [], []
        return total, dot([with_previous(last)], [last], stotal)

    @pl.loop(0, nx)
    def _(x):
        acc[...], accs[...] = slab(x, acc[...], accs[...])

    _, q = slab(None, None, accs[...])
    total = acc[...] - 0.125 * (q + q.T)
    live = jnp.broadcast_to(cnt[...], (rows, rows))
    keep = (lax.broadcasted_iota(jnp.int32, (rows, rows), 0) < live) & (
        lax.broadcasted_iota(jnp.int32, (rows, rows), 1) < live
    )
    own[...] = jnp.where(keep, total, 0.0)


def own(counts, vectors, stiff, diag):
    rows, nx, ny, nz = vectors.shape
    return pl.pallas_call(
        own_kernel,
        out_shape=jax.ShapeDtypeStruct((rows, rows), F32),
        in_specs=[VM] * 4,
        out_specs=VM,
        scratch_shapes=[
            pltpu.VMEM((rows * (ny + PAD), nz), F32),
            pltpu.VMEM((nx, ny, nz), F32),
            pltpu.VMEM((ny, rows, nz), BF),
            pltpu.VMEM((rows, rows), F32),
            pltpu.VMEM((rows, rows), F32),
        ],
        compiler_params=pltpu.CompilerParams(vmem_limit_bytes=16 * 2**20),
        cost_estimate=cost(2 * 10**9, 8 * 10**6),
        name="own",
    )(counts, vectors, stiff, diag)


def gram(left, right, n, total):
    for i in range(0, n, 2):
        total += lax.dot_general(
            jnp.concatenate([left[i], left[i + 1]], 1),
            jnp.concatenate([right[i], right[i + 1]], 1),
            NT,
            preferred_element_type=F32,
        )
    return total


def across_y_kernel(cnt, wya, wyb, wc, rya, ryb, faces, corners, two):
    nx, rows, _ = wya.shape
    x_even, y_even = even("sx"), even("sy")
    zero = jnp.zeros((rows, rows), F32)
    ya, yb = gram(wya, rya, nx, zero), gram(wyb, ryb, nx, zero)
    around = [
        [lax.dot_general(wc[2 * i + k], ry[nx + i], NT, preferred_element_type=F32) for k, ry in enumerate((rya, ryb))]
        for i in range(2)
    ]
    faces[:, 0:rows] = jnp.where(y_even, yb, ya)
    faces[:, rows : 2 * rows] = jnp.where(y_even, ya, yb)
    for ix in range(2):
        for iy in range(2):
            options = [jnp.where(y_even == (iy == 1), around[k][0], around[k][1]) for k in range(2)]
            i = 2 * ix + iy
            corners[:, i * rows : (i + 1) * rows] = jnp.where(x_even == (ix == 1), options[0], options[1])
    lane = lax.broadcasted_iota(jnp.int32, two.shape, 1)
    beside = rya[nx + 2].astype(F32)[0:8].astype(jnp.int32)
    two[...] = jnp.where(lane == 0, jnp.broadcast_to(cnt[...], two.shape), beside)


def across_y(counts, wya, wyb, wc, rya, ryb):
    rows, nz = wya.shape[1:]
    return pl.pallas_call(
        across_y_kernel,
        out_shape=(
            jax.ShapeDtypeStruct((rows, 2 * rows), F32),
            jax.ShapeDtypeStruct((rows, 4 * rows), F32),
            jax.ShapeDtypeStruct((8, nz), jnp.int32),
        ),
        in_specs=[VM] * 6,
        out_specs=(VM,) * 3,
        cost_estimate=cost(10**7, 10**6),
        compiler_params=pltpu.CompilerParams(vmem_limit_bytes=8 * 2**20),
        name="across_y",
    )(counts, wya, wyb, wc, rya, ryb)


def across_x_kernel(fy, wxa, wxb, rxa, rxb, faces):
    n, rows, _ = wxa.shape
    zero = jnp.zeros((rows, rows), F32)
    xa, xb = gram(wxa, rxa, n, zero), gram(wxb, rxb, n, zero)
    x_even = even("sx")
    faces[:, 0:rows] = jnp.where(x_even, xb, xa)
    faces[:, rows : 2 * rows] = jnp.where(x_even, xa, xb)
    faces[:, 2 * rows : 4 * rows] = fy[...]


def across_x(fy, wxa, wxb, rxa, rxb):
    rows = wxa.shape[1]
    return pl.pallas_call(
        across_x_kernel,
        out_shape=jax.ShapeDtypeStruct((rows, 4 * rows), F32),
        in_specs=[VM] * 5,
        out_specs=VM,
        cost_estimate=cost(10**8, 2 * 10**6),
        compiler_params=pltpu.CompilerParams(vmem_limit_bytes=8 * 2**20),
        name="across_x",
    )(fy, wxa, wxb, rxa, rxb)


def offset_kernel(masks, *refs):
    *known, offsets = refs
    me = lax.axis_index("sy")
    lane = lax.broadcasted_iota(jnp.int32, known[0].shape, 1)
    total = jnp.zeros(known[0].shape, F32)
    for one, mask in zip(known, masks):
        source = (me ^ mask) ^ lane
        total += jnp.where((lane < 2) & (source < me), one[...], 0).astype(F32)
    offsets[...] = jnp.sum(total, axis=1, keepdims=True)[0:1].astype(jnp.int32)


def offset_of(masks, known):
    return pl.pallas_call(
        lambda *refs: offset_kernel(masks, *refs),
        out_shape=jax.ShapeDtypeStruct((1, 1), jnp.int32),
        in_specs=[VM] * len(known),
        out_specs=VM,
        cost_estimate=cost(10**3, 10**4),
        compiler_params=pltpu.CompilerParams(vmem_limit_bytes=4 * 2**20),
        name="offset_of",
    )(*known)


def swap(values, axis, first):
    return lax.ppermute(values, axis, pairs(lax.axis_size(axis), first))


def on_device(vectors, root_stiff, diag_coef, counts):
    n_y = lax.axis_size("sy")
    fxa, fxb, fxc, fya, fyb = edges(counts, vectors, root_stiff)
    rxa = swap(fxa, "sx", 0)
    rxc = swap(fxc, "sx", 1)
    rxb = swap(fxb, "sx", 1)
    wxa, wxb, wya, wyb, wc = smooth(fxa, fxb, fya, fyb)
    mya, myb = pack(counts, fya, fyb, rxa, rxc)
    rya = swap(mya, "sy", 0)
    ryb = swap(myb, "sy", 1)
    own_block = own(counts, vectors, root_stiff, diag_coef)
    fy, corners, two = across_y(counts, wya, wyb, wc, rya, ryb)
    known, masks, bit = [two], [0], 2
    while bit < n_y:
        known += [lax.ppermute(one, "sy", [(i, i ^ bit) for i in range(n_y)]) for one in known]
        masks += [m ^ bit for m in masks]
        bit *= 2
    faces = across_x(fy, wxa, wxb, rxa, rxb)
    offsets = offset_of(tuple(masks), known)
    return own_block[None, None], faces[None, None], corners[None, None], offsets


def solution(mesh):
    assert mesh.shape["sy"] & (mesh.shape["sy"] - 1) == 0
    return jax.shard_map(
        on_device,
        mesh=mesh,
        in_specs=(
            P(None, "sx", "sy", None),
            P("sx", "sy", None),
            P("sx", "sy", None),
            P("sx", "sy"),
        ),
        out_specs=(
            P("sx", "sy", None, None),
            P("sx", "sy", None, None),
            P("sx", "sy", None, None),
            P("sx", "sy"),
        ),
        check_vma=False,
    )
```

```python
import jax
import jax.numpy as jnp
from jax import lax
from jax.experimental import pallas as pl
from jax.experimental.pallas import tpu as pltpu
from jax.sharding import PartitionSpec as P

F32 = jnp.float32
BF = jnp.bfloat16
NT = (((1,), (1,)), ((), ()))
NN = (((1,), (0,)), ((), ()))
PAD = 4
BAND = 8
VM = pl.BlockSpec(memory_space=pltpu.VMEM)
SM = pl.BlockSpec(memory_space=pltpu.SMEM)
ANY = pl.BlockSpec(memory_space=pl.ANY)
HBM = pl.BlockSpec(memory_space=pltpu.HBM)


def cost(flops, bytes_accessed):
    return pl.CostEstimate(flops=flops, bytes_accessed=bytes_accessed, transcendentals=0)


def tri(n, reps, scale):
    size = n * reps
    i = lax.broadcasted_iota(jnp.int32, (size, size), 0)
    j = lax.broadcasted_iota(jnp.int32, (size, size), 1)
    near = ((i // n) == (j // n)) & (jnp.abs(i - j) == 1)
    return (jnp.where(i == j, 1.0, jnp.where(near, 0.5, 0.0)) * scale).astype(BF)


def even(axis):
    return lax.rem(lax.axis_index(axis), 2) == 0


def pairs(count, first):
    steps = []
    for i in range(first, count - 1, 2):
        steps += [(i, i + 1), (i + 1, i)]
    return steps


def edge_kernel(cnt, v, s_any, fxa, fxb, fxc, fya, fyb, rx, ry, s, xbuf, ybuf, sem):
    rows, nx, ny, nz = v.shape
    stx, sty = ny + PAD, BAND + PAD
    x_even, y_even = even("sx"), even("sy")
    xa = jnp.where(x_even, nx - 1, 0)
    ya = jnp.where(y_even, ny - 1, 0)
    xb, yb = nx - 1 - xa, ny - 1 - ya
    bands = [pl.multiple_of((y // BAND) * BAND, BAND) for y in (ya, yb)]
    copies = [
        pltpu.make_async_copy(src, dst, sem.at[i])
        for i, (src, dst) in enumerate(
            (
                (s_any, s),
                (v.at[:, xb], xbuf.at[0]),
                (v.at[:, xa], xbuf.at[1]),
                (v.at[:, :, pl.ds(bands[0], BAND)], ybuf.at[0]),
                (v.at[:, :, pl.ds(bands[1], BAND)], ybuf.at[1]),
            )
        )
    ]
    for c in copies:
        c.start()
    live = lax.broadcasted_iota(jnp.int32, (rows, nz), 0) < jnp.broadcast_to(cnt[...], (rows, nz))

    def scaled(m, stiff):
        return jnp.where(live, m * jnp.broadcast_to(stiff, (rows, nz)), 0.0).astype(BF)

    copies[0].wait()
    for i, (x, out) in enumerate(((xb, fxb), (xa, fxa))):
        copies[1 + i].wait()
        for a in range(rows):
            rx[a * stx : a * stx + ny, :] = xbuf[i, a].astype(F32)
        for y in range(ny):
            out[y] = scaled(rx[pl.ds(y, rows, stride=stx), :], s[x, pl.ds(y, 1), :])
    fxc[0] = fxb[ya]
    fxc[1] = fxb[yb]
    for i, (y, out) in enumerate(((ya, fya), (yb, fyb))):
        copies[3 + i].wait()
        inner = y - bands[i]
        for x in range(nx):
            for a in range(rows):
                ry[x, a * sty : a * sty + BAND, :] = ybuf[i, a, x].astype(F32)
            out[x] = scaled(ry[x, pl.ds(inner, rows, stride=sty), :], s[x, pl.ds(y, 1), :])


def edges(counts, vectors, stiff):
    rows, nx, ny, nz = vectors.shape
    face = lambda n: jax.ShapeDtypeStruct((n, rows, nz), BF)
    return pl.pallas_call(
        edge_kernel,
        out_shape=(face(ny), face(ny), face(2), face(nx), face(nx)),
        in_specs=[VM, HBM, HBM],
        out_specs=(VM,) * 5,
        scratch_shapes=[
            pltpu.VMEM((rows * (ny + PAD), nz), F32),
            pltpu.VMEM((nx, rows * (BAND + PAD), nz), F32),
            pltpu.VMEM(stiff.shape, F32),
            pltpu.VMEM((2, rows, ny, nz), BF),
            pltpu.VMEM((2, rows, nx, BAND, nz), BF),
            pltpu.SemaphoreType.DMA((5,)),
        ],
        cost_estimate=cost(10**6, 4 * 10**6),
        compiler_params=pltpu.CompilerParams(vmem_limit_bytes=52 * 2**20),
        name="edges",
    )(counts, vectors, stiff)


def pack_kernel(cnt, fya, fyb, rxa, rxc, mya, myb):
    nx, rows, nz = fya.shape
    ny = rxa.shape[0]
    hi = jnp.where(even("sy"), ny - 1, 0)
    count = jnp.broadcast_to(cnt[...].astype(F32), (rows, nz)).astype(BF)
    for i, (src, y, out) in enumerate(((fya, hi, mya), (fyb, ny - 1 - hi, myb))):
        out[0:nx] = src[...]
        out[nx] = rxa[y]
        out[nx + 1] = rxc[i]
        out[nx + 2] = count


def pack(counts, fya, fyb, rxa, rxc):
    nx, rows, nz = fya.shape
    out = jax.ShapeDtypeStruct((nx + 3, rows, nz), BF)
    return pl.pallas_call(
        pack_kernel,
        out_shape=(out, out),
        in_specs=[VM] * 5,
        out_specs=(VM, VM),
        cost_estimate=cost(10**5, 10**6),
        compiler_params=pltpu.CompilerParams(vmem_limit_bytes=8 * 2**20),
        name="pack",
    )(counts, fya, fyb, rxa, rxc)


def along_z(stack, n, stencil):
    rows, nz = stack(0).shape
    wide = jnp.concatenate([jnp.concatenate([stack(2 * c), stack(2 * c + 1)], 1) for c in range(n // 2)], 0)
    z = lax.dot_general(wide, stencil, NN, preferred_element_type=F32)
    return [z[(i // 2) * rows : (i // 2 + 1) * rows, (i % 2) * nz : (i % 2 + 1) * nz] for i in range(n)]


def smooth_kernel(fxa, fxb, fya, fyb, wxa, wxb, wya, wyb, wc):
    ny, _, nz = fxa.shape
    stencil = tri(nz, 2, -0.25)
    for src, out in ((fxa, wxa), (fxb, wxb), (fya, wya), (fyb, wyb)):
        n = src.shape[0]
        zs = along_z(lambda i: src[i], n, stencil)
        for i in range(n):
            t = zs[i] + zs[i]
            if i > 0:
                t = t + zs[i - 1]
            if i < n - 1:
                t = t + zs[i + 1]
            out[i] = t.astype(BF)
    y_even = even("sy")
    rows_y = (jnp.where(y_even, ny - 1, 0), jnp.where(y_even, 0, ny - 1))
    for i, src in enumerate((fxa, fxb)):
        zs = along_z(lambda k: src[rows_y[k]], 2, stencil)
        for k in range(2):
            wc[2 * i + k] = zs[k].astype(BF)


def smooth(fxa, fxb, fya, fyb):
    ny, rows, nz = fxa.shape
    nx = fya.shape[0]
    face = lambda n: jax.ShapeDtypeStruct((n, rows, nz), BF)
    return pl.pallas_call(
        smooth_kernel,
        out_shape=(face(ny), face(ny), face(nx), face(nx), face(4)),
        in_specs=[VM] * 4,
        out_specs=(VM,) * 5,
        cost_estimate=cost(10**8, 2 * 10**6),
        compiler_params=pltpu.CompilerParams(vmem_limit_bytes=12 * 2**20),
        name="smooth",
    )(fxa, fxb, fya, fyb)


def own_kernel(first, stop, v, s, d, ubuf, acc, accs, r, er):
    rows, _, ny, nz = v.shape
    st = ny + PAD
    er[...] = d[...] + s[...] * s[...]
    inner = jnp.where(lax.broadcasted_iota(jnp.int32, (rows, nz), 1) == 0, 0.0, 1.0).astype(BF)

    def with_previous(p):
        return p + pltpu.roll(p, 1, 1) * inner

    def dot(left, right, total):
        return total + lax.dot_general(
            jnp.concatenate(left, 1), jnp.concatenate(right, 1), NT, preferred_element_type=F32
        )

    def slab(x, total, stotal):
        if x is not None:
            for a in range(rows):
                r[a * st : a * st + ny, :] = v[a, x].astype(F32)
        last = None
        left, right, ps = [], [], []
        for y in range(ny):
            if x is not None:
                m = r[pl.ds(y, rows, stride=st), :]
                u = (m * jnp.broadcast_to(s[x, pl.ds(y, 1), :], (rows, nz))).astype(BF)
                left.append((m * jnp.broadcast_to(er[x, pl.ds(y, 1), :], (rows, nz))).astype(BF))
                right.append(m.astype(BF))
                both = u + ubuf[y]
                ubuf[y] = u
            else:
                both = ubuf[y]
            ps.append(both if last is None else both + last)
            last = both
            if y % 2:
                if x is not None:
                    total = dot(left, right, total)
                stotal = dot([with_previous(p) for p in ps], ps, stotal)
                left, right, ps = [], [], []
        return total, dot([with_previous(last)], [last], stotal)

    @pl.loop(first, stop)
    def _(x):
        acc[...], accs[...] = slab(x, acc[...], accs[...])

    return slab


def own_begin_kernel(stop, v, s, d, ubuf, acc, accs, r, er):
    for ref in (ubuf, acc, accs):
        ref[...] = jnp.zeros_like(ref)
    own_kernel(0, stop, v, s, d, ubuf, acc, accs, r, er)


def own_end_kernel(first, cnt, v, s, d, ubuf0, acc0, accs0, own, ubuf, acc, accs, r, er):
    for src, ref in ((ubuf0, ubuf), (acc0, acc), (accs0, accs)):
        ref[...] = src[...]
    rows, nx = v.shape[:2]
    slab = own_kernel(first, nx, v, s, d, ubuf, acc, accs, r, er)
    _, q = slab(None, None, accs[...])
    total = acc[...] - 0.125 * (q + q.T)
    live = jnp.broadcast_to(cnt[...], (rows, rows))
    keep = (lax.broadcasted_iota(jnp.int32, (rows, rows), 0) < live) & (
        lax.broadcasted_iota(jnp.int32, (rows, rows), 1) < live
    )
    own[...] = jnp.where(keep, total, 0.0)


def own_parts(vectors):
    rows, nx, ny, nz = vectors.shape
    state = [((ny, rows, nz), BF), ((rows, rows), F32), ((rows, rows), F32)]
    work = [pltpu.VMEM((rows * (ny + PAD), nz), F32), pltpu.VMEM((nx, ny, nz), F32)]
    params = dict(
        cost_estimate=cost(10**9, 5 * 10**6),
        compiler_params=pltpu.CompilerParams(vmem_limit_bytes=16 * 2**20),
    )
    return state, work, params


def own_begin(cut, vectors, stiff, diag):
    state, work, params = own_parts(vectors)
    return pl.pallas_call(
        lambda *refs: own_begin_kernel(cut, *refs),
        out_shape=tuple(jax.ShapeDtypeStruct(*one) for one in state),
        in_specs=[VM] * 3,
        out_specs=(VM,) * 3,
        scratch_shapes=work,
        name="own_begin",
        **params,
    )(vectors, stiff, diag)


def own_end(cut, counts, vectors, stiff, diag, so_far):
    state, work, params = own_parts(vectors)
    rows = vectors.shape[0]
    return pl.pallas_call(
        lambda *refs: own_end_kernel(cut, *refs),
        out_shape=jax.ShapeDtypeStruct((rows, rows), F32),
        in_specs=[VM] * 7,
        out_specs=VM,
        scratch_shapes=[pltpu.VMEM(*one) for one in state] + work,
        name="own_end",
        **params,
    )(counts, vectors, stiff, diag, *so_far)


def gram(left, right, n, total):
    for i in range(0, n, 2):
        total += lax.dot_general(
            jnp.concatenate([left[i], left[i + 1]], 1),
            jnp.concatenate([right[i], right[i + 1]], 1),
            NT,
            preferred_element_type=F32,
        )
    return total


def across_y_kernel(masks, fx, wya, wyb, wc, rya, ryb, *rest):
    *known, faces, corners, offsets = rest
    nx, rows, _ = wya.shape
    x_even, y_even = even("sx"), even("sy")
    zero = jnp.zeros((rows, rows), F32)
    ya, yb = gram(wya, rya, nx, zero), gram(wyb, ryb, nx, zero)
    around = [
        [lax.dot_general(wc[2 * i + k], ry[nx + i], NT, preferred_element_type=F32) for k, ry in enumerate((rya, ryb))]
        for i in range(2)
    ]
    faces[:, 0 : 2 * rows] = fx[...]
    faces[:, 2 * rows : 3 * rows] = jnp.where(y_even, yb, ya)
    faces[:, 3 * rows : 4 * rows] = jnp.where(y_even, ya, yb)
    offset_kernel(masks, *known, offsets)
    for ix in range(2):
        for iy in range(2):
            options = [jnp.where(y_even == (iy == 1), around[k][0], around[k][1]) for k in range(2)]
            i = 2 * ix + iy
            corners[:, i * rows : (i + 1) * rows] = jnp.where(x_even == (ix == 1), options[0], options[1])


def two_kernel(cnt, rya, two):
    lane = lax.broadcasted_iota(jnp.int32, two.shape, 1)
    beside = rya[rya.shape[0] - 1].astype(F32)[0 : two.shape[0]].astype(jnp.int32)
    two[...] = jnp.where(lane == 0, jnp.broadcast_to(cnt[...], two.shape), beside)


def two_counts(counts, rya):
    return pl.pallas_call(
        two_kernel,
        out_shape=jax.ShapeDtypeStruct((8, rya.shape[2]), jnp.int32),
        in_specs=[VM] * 2,
        out_specs=VM,
        cost_estimate=cost(10**4, 10**4),
        compiler_params=pltpu.CompilerParams(vmem_limit_bytes=8 * 2**20),
        name="two_counts",
    )(counts, rya)


def across_y(masks, fx, wya, wyb, wc, rya, ryb, known):
    rows = wya.shape[1]
    return pl.pallas_call(
        lambda *refs: across_y_kernel(masks, *refs),
        out_shape=(
            jax.ShapeDtypeStruct((rows, 4 * rows), F32),
            jax.ShapeDtypeStruct((rows, 4 * rows), F32),
            jax.ShapeDtypeStruct((1, 1), jnp.int32),
        ),
        in_specs=[VM] * (6 + len(known)),
        out_specs=(VM,) * 3,
        cost_estimate=cost(10**7, 10**6),
        compiler_params=pltpu.CompilerParams(vmem_limit_bytes=8 * 2**20),
        name="across_y",
    )(fx, wya, wyb, wc, rya, ryb, *known)


def across_x_kernel(wxa, wxb, rxa, rxb, faces):
    n, rows, _ = wxa.shape
    zero = jnp.zeros((rows, rows), F32)
    xa, xb = gram(wxa, rxa, n, zero), gram(wxb, rxb, n, zero)
    x_even = even("sx")
    faces[:, 0:rows] = jnp.where(x_even, xb, xa)
    faces[:, rows : 2 * rows] = jnp.where(x_even, xa, xb)


def across_x(wxa, wxb, rxa, rxb):
    rows = wxa.shape[1]
    return pl.pallas_call(
        across_x_kernel,
        out_shape=jax.ShapeDtypeStruct((rows, 2 * rows), F32),
        in_specs=[VM] * 4,
        out_specs=VM,
        cost_estimate=cost(10**8, 2 * 10**6),
        compiler_params=pltpu.CompilerParams(vmem_limit_bytes=8 * 2**20),
        name="across_x",
    )(wxa, wxb, rxa, rxb)


def offset_kernel(masks, *refs):
    *known, offsets = refs
    me = lax.axis_index("sy")
    lane = lax.broadcasted_iota(jnp.int32, known[0].shape, 1)
    total = jnp.zeros(known[0].shape, F32)
    for one, mask in zip(known, masks):
        source = (me ^ mask) ^ lane
        total += jnp.where((lane < 2) & (source < me), one[...], 0).astype(F32)
    offsets[...] = jnp.sum(total, axis=1, keepdims=True)[0:1].astype(jnp.int32)


def swap(values, axis, first):
    return lax.ppermute(values, axis, pairs(lax.axis_size(axis), first))


def on_device(vectors, root_stiff, diag_coef, counts):
    n_y = lax.axis_size("sy")
    fxa, fxb, fxc, fya, fyb = edges(counts, vectors, root_stiff)
    rxc = swap(fxc, "sx", 1)
    rxb = swap(fxb, "sx", 1)
    rxa = swap(fxa, "sx", 0)
    wxa, wxb, wya, wyb, wc = smooth(fxa, fxb, fya, fyb)
    mya, myb = pack(counts, fya, fyb, rxa, rxc)
    rya = swap(mya, "sy", 0)
    cut = vectors.shape[1] // 2
    so_far = own_begin(cut, vectors, root_stiff, diag_coef)
    ryb = swap(myb, "sy", 1)
    two = two_counts(counts, rya)
    known, masks, bit = [two], [0], 2
    while bit < n_y:
        known += [lax.ppermute(one, "sy", [(i, i ^ bit) for i in range(n_y)]) for one in known]
        masks += [m ^ bit for m in masks]
        bit *= 2
    own_block = own_end(cut, counts, vectors, root_stiff, diag_coef, so_far)
    fx = across_x(wxa, wxb, rxa, rxb)
    faces, corners, offsets = across_y(tuple(masks), fx, wya, wyb, wc, rya, ryb, known)
    return own_block[None, None], faces[None, None], corners[None, None], offsets


def solution(mesh):
    assert mesh.shape["sy"] & (mesh.shape["sy"] - 1) == 0
    return jax.shard_map(
        on_device,
        mesh=mesh,
        in_specs=(
            P(None, "sx", "sy", None),
            P("sx", "sy", None),
            P("sx", "sy", None),
            P("sx", "sy"),
        ),
        out_specs=(
            P("sx", "sy", None, None),
            P("sx", "sy", None, None),
            P("sx", "sy", None, None),
            P("sx", "sy"),
        ),
        check_vma=False,
    )
```

```python
import jax
import jax.numpy as jnp
from jax import lax
from jax.experimental import pallas as pl
from jax.experimental.pallas import tpu as pltpu
from jax.sharding import PartitionSpec as P

F32 = jnp.float32
BF = jnp.bfloat16
NT = (((1,), (1,)), ((), ()))
NN = (((1,), (0,)), ((), ()))
PAD = 4
BAND = 8
VM = pl.BlockSpec(memory_space=pltpu.VMEM)
SM = pl.BlockSpec(memory_space=pltpu.SMEM)
ANY = pl.BlockSpec(memory_space=pl.ANY)
HBM = pl.BlockSpec(memory_space=pltpu.HBM)


def cost(flops, bytes_accessed):
    return pl.CostEstimate(flops=flops, bytes_accessed=bytes_accessed, transcendentals=0)


def tri(n, reps, scale):
    size = n * reps
    i = lax.broadcasted_iota(jnp.int32, (size, size), 0)
    j = lax.broadcasted_iota(jnp.int32, (size, size), 1)
    near = ((i // n) == (j // n)) & (jnp.abs(i - j) == 1)
    return (jnp.where(i == j, 1.0, jnp.where(near, 0.5, 0.0)) * scale).astype(BF)


def even(axis):
    return lax.rem(lax.axis_index(axis), 2) == 0


def pairs(count, first):
    steps = []
    for i in range(first, count - 1, 2):
        steps += [(i, i + 1), (i + 1, i)]
    return steps


def edge_kernel(cnt, v, s_any, fxa, fxb, fxc, fya, fyb, rx, ry, s, xbuf, ybuf, sem):
    rows, nx, ny, nz = v.shape
    stx, sty = ny + PAD, BAND + PAD
    x_even, y_even = even("sx"), even("sy")
    xa = jnp.where(x_even, nx - 1, 0)
    ya = jnp.where(y_even, ny - 1, 0)
    xb, yb = nx - 1 - xa, ny - 1 - ya
    bands = [pl.multiple_of((y // BAND) * BAND, BAND) for y in (ya, yb)]
    copies = [
        pltpu.make_async_copy(src, dst, sem.at[i])
        for i, (src, dst) in enumerate(
            (
                (s_any, s),
                (v.at[:, xb], xbuf.at[0]),
                (v.at[:, xa], xbuf.at[1]),
                (v.at[:, :, pl.ds(bands[0], BAND)], ybuf.at[0]),
                (v.at[:, :, pl.ds(bands[1], BAND)], ybuf.at[1]),
            )
        )
    ]
    for c in copies:
        c.start()
    live = lax.broadcasted_iota(jnp.int32, (rows, nz), 0) < jnp.broadcast_to(cnt[...], (rows, nz))

    def scaled(m, stiff):
        return jnp.where(live, m * jnp.broadcast_to(stiff, (rows, nz)), 0.0).astype(BF)

    copies[0].wait()
    for i, (x, out) in enumerate(((xb, fxb), (xa, fxa))):
        copies[1 + i].wait()
        for a in range(rows):
            rx[a * stx : a * stx + ny, :] = xbuf[i, a].astype(F32)
        for y in range(ny):
            row = scaled(rx[pl.ds(y, rows, stride=stx), :], s[x, pl.ds(y, 1), :])
            if i == 1:
                out[y] = row
            elif 0 < y < ny - 1:
                out[y - 1] = row
            else:
                fxc[jnp.where(ya == y, 0, 1)] = row
    for i, (y, out) in enumerate(((ya, fya), (yb, fyb))):
        copies[3 + i].wait()
        inner = y - bands[i]
        for x in range(nx):
            for a in range(rows):
                ry[x, a * sty : a * sty + BAND, :] = ybuf[i, a, x].astype(F32)
            out[x] = scaled(ry[x, pl.ds(inner, rows, stride=sty), :], s[x, pl.ds(y, 1), :])


def edges(counts, vectors, stiff):
    rows, nx, ny, nz = vectors.shape
    face = lambda n: jax.ShapeDtypeStruct((n, rows, nz), BF)
    return pl.pallas_call(
        edge_kernel,
        out_shape=(face(ny), face(ny - 2), face(2), face(nx), face(nx)),
        in_specs=[VM, HBM, HBM],
        out_specs=(VM,) * 5,
        scratch_shapes=[
            pltpu.VMEM((rows * (ny + PAD), nz), F32),
            pltpu.VMEM((nx, rows * (BAND + PAD), nz), F32),
            pltpu.VMEM(stiff.shape, F32),
            pltpu.VMEM((2, rows, ny, nz), BF),
            pltpu.VMEM((2, rows, nx, BAND, nz), BF),
            pltpu.SemaphoreType.DMA((5,)),
        ],
        cost_estimate=cost(10**6, 4 * 10**6),
        compiler_params=pltpu.CompilerParams(vmem_limit_bytes=52 * 2**20),
        name="edges",
    )(counts, vectors, stiff)


def pack_kernel(cnt, fya, fyb, rxa, rxc, mya, myb):
    nx, rows, nz = fya.shape
    ny = rxa.shape[0]
    hi = jnp.where(even("sy"), ny - 1, 0)
    count = jnp.broadcast_to(cnt[...].astype(F32), (rows, nz)).astype(BF)
    for i, (src, y, out) in enumerate(((fya, hi, mya), (fyb, ny - 1 - hi, myb))):
        out[0:nx] = src[...]
        out[nx] = rxa[y]
        out[nx + 1] = rxc[i]
        out[nx + 2] = count


def pack(counts, fya, fyb, rxa, rxc):
    nx, rows, nz = fya.shape
    out = jax.ShapeDtypeStruct((nx + 3, rows, nz), BF)
    return pl.pallas_call(
        pack_kernel,
        out_shape=(out, out),
        in_specs=[VM] * 5,
        out_specs=(VM, VM),
        cost_estimate=cost(10**5, 10**6),
        compiler_params=pltpu.CompilerParams(vmem_limit_bytes=8 * 2**20),
        name="pack",
    )(counts, fya, fyb, rxa, rxc)


def along_z(stack, n, stencil):
    rows, nz = stack(0).shape
    wide = jnp.concatenate([jnp.concatenate([stack(2 * c), stack(2 * c + 1)], 1) for c in range(n // 2)], 0)
    z = lax.dot_general(wide, stencil, NN, preferred_element_type=F32)
    return [z[(i // 2) * rows : (i // 2 + 1) * rows, (i % 2) * nz : (i % 2 + 1) * nz] for i in range(n)]


def smooth_kernel(fxa, fxb, fxc, fya, fyb, wxa, wxb, wxe, wya, wyb, wc):
    ny, _, nz = fxa.shape
    stencil = tri(nz, 2, -0.25)
    y_even = even("sy")
    first, last = jnp.where(y_even, 1, 0), jnp.where(y_even, 0, 1)

    def put_xb(i, value):
        if 0 < i < ny - 1:
            wxb[i - 1] = value
        else:
            wxe[first if i == 0 else last] = value

    def get_xb(i):
        return fxb[i - 1] if 0 < i < ny - 1 else fxc[first if i == 0 else last]

    def getter(ref):
        return lambda i: ref[i]

    def putter(ref):
        def put(i, value):
            ref[i] = value

        return put

    for n, get, put in (
        (ny, getter(fxa), putter(wxa)),
        (ny, get_xb, put_xb),
        (fya.shape[0], getter(fya), putter(wya)),
        (fyb.shape[0], getter(fyb), putter(wyb)),
    ):
        zs = along_z(get, n, stencil)
        for i in range(n):
            t = zs[i] + zs[i]
            if i > 0:
                t = t + zs[i - 1]
            if i < n - 1:
                t = t + zs[i + 1]
            put(i, t.astype(BF))
    rows_y = (jnp.where(y_even, ny - 1, 0), jnp.where(y_even, 0, ny - 1))
    for i, get in enumerate((lambda k: fxa[rows_y[k]], lambda k: fxc[k])):
        zs = along_z(get, 2, stencil)
        for k in range(2):
            wc[2 * i + k] = zs[k].astype(BF)


def smooth(fxa, fxb, fxc, fya, fyb):
    ny, rows, nz = fxa.shape
    nx = fya.shape[0]
    face = lambda n: jax.ShapeDtypeStruct((n, rows, nz), BF)
    return pl.pallas_call(
        smooth_kernel,
        out_shape=(face(ny), face(ny - 2), face(2), face(nx), face(nx), face(4)),
        in_specs=[VM] * 5,
        out_specs=(VM,) * 6,
        cost_estimate=cost(10**8, 2 * 10**6),
        compiler_params=pltpu.CompilerParams(vmem_limit_bytes=12 * 2**20),
        name="smooth",
    )(fxa, fxb, fxc, fya, fyb)


def own_kernel(first, stop, v, s, d, ubuf, acc, accs, r, er):
    rows, _, ny, nz = v.shape
    st = ny + PAD
    er[...] = d[...] + s[...] * s[...]
    inner = jnp.where(lax.broadcasted_iota(jnp.int32, (rows, nz), 1) == 0, 0.0, 1.0).astype(BF)

    def with_previous(p):
        return p + pltpu.roll(p, 1, 1) * inner

    def dot(left, right, total):
        return total + lax.dot_general(
            jnp.concatenate(left, 1), jnp.concatenate(right, 1), NT, preferred_element_type=F32
        )

    def slab(x, total, stotal):
        if x is not None:
            for a in range(rows):
                r[a * st : a * st + ny, :] = v[a, x].astype(F32)
        last = None
        left, right, ps = [], [], []
        for y in range(ny):
            if x is not None:
                m = r[pl.ds(y, rows, stride=st), :]
                u = (m * jnp.broadcast_to(s[x, pl.ds(y, 1), :], (rows, nz))).astype(BF)
                left.append((m * jnp.broadcast_to(er[x, pl.ds(y, 1), :], (rows, nz))).astype(BF))
                right.append(m.astype(BF))
                both = u + ubuf[y]
                ubuf[y] = u
            else:
                both = ubuf[y]
            ps.append(both if last is None else both + last)
            last = both
            if y % 2:
                if x is not None:
                    total = dot(left, right, total)
                stotal = dot([with_previous(p) for p in ps], ps, stotal)
                left, right, ps = [], [], []
        return total, dot([with_previous(last)], [last], stotal)

    @pl.loop(first, stop)
    def _(x):
        acc[...], accs[...] = slab(x, acc[...], accs[...])

    return slab


def own_begin_kernel(stop, v, s, d, ubuf, acc, accs, r, er):
    for ref in (ubuf, acc, accs):
        ref[...] = jnp.zeros_like(ref)
    own_kernel(0, stop, v, s, d, ubuf, acc, accs, r, er)


def own_end_kernel(first, cnt, v, s, d, ubuf0, acc0, accs0, own, ubuf, acc, accs, r, er):
    for src, ref in ((ubuf0, ubuf), (acc0, acc), (accs0, accs)):
        ref[...] = src[...]
    rows, nx = v.shape[:2]
    slab = own_kernel(first, nx, v, s, d, ubuf, acc, accs, r, er)
    _, q = slab(None, None, accs[...])
    total = acc[...] - 0.125 * (q + q.T)
    live = jnp.broadcast_to(cnt[...], (rows, rows))
    keep = (lax.broadcasted_iota(jnp.int32, (rows, rows), 0) < live) & (
        lax.broadcasted_iota(jnp.int32, (rows, rows), 1) < live
    )
    own[...] = jnp.where(keep, total, 0.0)


def own_parts(vectors):
    rows, nx, ny, nz = vectors.shape
    state = [((ny, rows, nz), BF), ((rows, rows), F32), ((rows, rows), F32)]
    work = [pltpu.VMEM((rows * (ny + PAD), nz), F32), pltpu.VMEM((nx, ny, nz), F32)]
    params = dict(
        cost_estimate=cost(10**9, 5 * 10**6),
        compiler_params=pltpu.CompilerParams(vmem_limit_bytes=16 * 2**20),
    )
    return state, work, params


def own_begin(cut, vectors, stiff, diag):
    state, work, params = own_parts(vectors)
    return pl.pallas_call(
        lambda *refs: own_begin_kernel(cut, *refs),
        out_shape=tuple(jax.ShapeDtypeStruct(*one) for one in state),
        in_specs=[VM] * 3,
        out_specs=(VM,) * 3,
        scratch_shapes=work,
        name="own_begin",
        **params,
    )(vectors, stiff, diag)


def own_end(cut, counts, vectors, stiff, diag, so_far):
    state, work, params = own_parts(vectors)
    rows = vectors.shape[0]
    return pl.pallas_call(
        lambda *refs: own_end_kernel(cut, *refs),
        out_shape=jax.ShapeDtypeStruct((rows, rows), F32),
        in_specs=[VM] * 7,
        out_specs=VM,
        scratch_shapes=[pltpu.VMEM(*one) for one in state] + work,
        name="own_end",
        **params,
    )(counts, vectors, stiff, diag, *so_far)


def gram(left, right, n, total):
    for i in range(0, n, 2):
        total += lax.dot_general(
            jnp.concatenate([left[i], left[i + 1]], 1),
            jnp.concatenate([right[i], right[i + 1]], 1),
            NT,
            preferred_element_type=F32,
        )
    return total


def across_y_kernel(masks, fx, wya, wyb, wc, rya, ryb, *rest):
    *known, faces, corners, offsets = rest
    nx, rows, _ = wya.shape
    x_even, y_even = even("sx"), even("sy")
    zero = jnp.zeros((rows, rows), F32)
    ya, yb = gram(wya, rya, nx, zero), gram(wyb, ryb, nx, zero)
    around = [
        [lax.dot_general(wc[2 * i + k], ry[nx + i], NT, preferred_element_type=F32) for k, ry in enumerate((rya, ryb))]
        for i in range(2)
    ]
    faces[:, 0 : 2 * rows] = fx[...]
    faces[:, 2 * rows : 3 * rows] = jnp.where(y_even, yb, ya)
    faces[:, 3 * rows : 4 * rows] = jnp.where(y_even, ya, yb)
    offset_kernel(masks, *known, offsets)
    for ix in range(2):
        for iy in range(2):
            options = [jnp.where(y_even == (iy == 1), around[k][0], around[k][1]) for k in range(2)]
            i = 2 * ix + iy
            corners[:, i * rows : (i + 1) * rows] = jnp.where(x_even == (ix == 1), options[0], options[1])


def two_kernel(cnt, rya, two):
    lane = lax.broadcasted_iota(jnp.int32, two.shape, 1)
    beside = rya[rya.shape[0] - 1].astype(F32)[0 : two.shape[0]].astype(jnp.int32)
    two[...] = jnp.where(lane == 0, jnp.broadcast_to(cnt[...], two.shape), beside)


def two_counts(counts, rya):
    return pl.pallas_call(
        two_kernel,
        out_shape=jax.ShapeDtypeStruct((8, rya.shape[2]), jnp.int32),
        in_specs=[VM] * 2,
        out_specs=VM,
        cost_estimate=cost(10**4, 10**4),
        compiler_params=pltpu.CompilerParams(vmem_limit_bytes=8 * 2**20),
        name="two_counts",
    )(counts, rya)


def across_y(masks, fx, wya, wyb, wc, rya, ryb, known):
    rows = wya.shape[1]
    return pl.pallas_call(
        lambda *refs: across_y_kernel(masks, *refs),
        out_shape=(
            jax.ShapeDtypeStruct((rows, 4 * rows), F32),
            jax.ShapeDtypeStruct((rows, 4 * rows), F32),
            jax.ShapeDtypeStruct((1, 1), jnp.int32),
        ),
        in_specs=[VM] * (6 + len(known)),
        out_specs=(VM,) * 3,
        cost_estimate=cost(10**7, 10**6),
        compiler_params=pltpu.CompilerParams(vmem_limit_bytes=8 * 2**20),
        name="across_y",
    )(fx, wya, wyb, wc, rya, ryb, *known)


def across_x_kernel(wxa, wxb, wxe, rxa, rxb, rxc, faces):
    n, rows, _ = wxa.shape
    zero = jnp.zeros((rows, rows), F32)
    xa = gram(wxa, rxa, n, zero)
    xb = gram(wxb, rxb, n - 2, gram(wxe, rxc, 2, zero))
    x_even = even("sx")
    faces[:, 0:rows] = jnp.where(x_even, xb, xa)
    faces[:, rows : 2 * rows] = jnp.where(x_even, xa, xb)


def across_x(wxa, wxb, wxe, rxa, rxb, rxc):
    rows = wxa.shape[1]
    return pl.pallas_call(
        across_x_kernel,
        out_shape=jax.ShapeDtypeStruct((rows, 2 * rows), F32),
        in_specs=[VM] * 6,
        out_specs=VM,
        cost_estimate=cost(10**8, 2 * 10**6),
        compiler_params=pltpu.CompilerParams(vmem_limit_bytes=8 * 2**20),
        name="across_x",
    )(wxa, wxb, wxe, rxa, rxb, rxc)


def offset_kernel(masks, *refs):
    *known, offsets = refs
    me = lax.axis_index("sy")
    lane = lax.broadcasted_iota(jnp.int32, known[0].shape, 1)
    total = jnp.zeros(known[0].shape, F32)
    for one, mask in zip(known, masks):
        source = (me ^ mask) ^ lane
        total += jnp.where((lane < 2) & (source < me), one[...], 0).astype(F32)
    offsets[...] = jnp.sum(total, axis=1, keepdims=True)[0:1].astype(jnp.int32)


def swap(values, axis, first):
    return lax.ppermute(values, axis, pairs(lax.axis_size(axis), first))


def on_device(vectors, root_stiff, diag_coef, counts):
    n_y = lax.axis_size("sy")
    fxa, fxb, fxc, fya, fyb = edges(counts, vectors, root_stiff)
    rxc = swap(fxc, "sx", 1)
    rxb = swap(fxb, "sx", 1)
    rxa = swap(fxa, "sx", 0)
    wxa, wxb, wxe, wya, wyb, wc = smooth(fxa, fxb, fxc, fya, fyb)
    mya, myb = pack(counts, fya, fyb, rxa, rxc)
    rya = swap(mya, "sy", 0)
    cut = vectors.shape[1] * 5 // 8
    so_far = own_begin(cut, vectors, root_stiff, diag_coef)
    ryb = swap(myb, "sy", 1)
    two = two_counts(counts, rya)
    known, masks, bit = [two], [0], 2
    while bit < n_y:
        known += [lax.ppermute(one, "sy", [(i, i ^ bit) for i in range(n_y)]) for one in known]
        masks += [m ^ bit for m in masks]
        bit *= 2
    own_block = own_end(cut, counts, vectors, root_stiff, diag_coef, so_far)
    fx = across_x(wxa, wxb, wxe, rxa, rxb, rxc)
    faces, corners, offsets = across_y(tuple(masks), fx, wya, wyb, wc, rya, ryb, known)
    return own_block[None, None], faces[None, None], corners[None, None], offsets


def solution(mesh):
    assert mesh.shape["sy"] & (mesh.shape["sy"] - 1) == 0
    return jax.shard_map(
        on_device,
        mesh=mesh,
        in_specs=(
            P(None, "sx", "sy", None),
            P("sx", "sy", None),
            P("sx", "sy", None),
            P("sx", "sy"),
        ),
        out_specs=(
            P("sx", "sy", None, None),
            P("sx", "sy", None, None),
            P("sx", "sy", None, None),
            P("sx", "sy"),
        ),
        check_vma=False,
    )
```
